32 devices in a mesh: leaf: 16 (over z, x, core), head: 2 (over y).
Axes of the slice: x: 2, y: 2, z: 4, core: 2. Of those that a mesh axis runs over, the one named last changes fastest.
Arguments:
- queries: bfloat16 [4096, 2048], P(('leaf', 'head')), may hold values from -64 to 64
- keys: bfloat16 [4096, 256], P(('leaf', 'head')), may hold values from -16 to 16
- values: bfloat16 [4096, 256], P(('leaf', 'head')), may hold values from -6 to 6
- output_gradient: bfloat16 [4096, 2048], P('leaf', 'head'), may hold values from -6 to 6
- parents: int32 [16], replicated, may hold values from -1 to 15, as said below
Outputs:
- attended: bfloat16 [4096, 2048], P('leaf', 'head')
- query_gradient: bfloat16 [4096, 2048], P(('leaf', 'head'))
- key_grad: bfloat16 [4096, 256], P(('leaf', 'head'))
- value_grad: bfloat16 [4096, 256], P(('leaf', 'head'))
The draws below stay inside these ranges and needn't reach their ends.
Inputs may be any that keep to these rules, and one draw needn't show every extreme that they name: Exactly one group has parent -1; every other group's parent is another group, and following parents from any group reaches that root after at most 6 steps; some group is exactly 6 steps from it.
All inputs are finite; a program needn't handle non-finite values.
Results may differ from the reference program's by a relative error of at most 0.035.
Values may be sent and summed in bfloat16 or wider, within the bound.
No kernel may reach another device: no remote copies, remote signals or barrier semaphores. Data moves between devices by JAX's collectives and lax.ppermute only.
A program may use at most 64 MiB of HBM per device.

```python
import math
import jax
import jax.numpy as jnp
from jax import lax

HEAD_SIZE = 128
QUERIES_PER_KEY = 8
NODE_TOKENS = 128
NODES_PER_GROUP = 2
MAX_DEPTH = 6
KEY_HEADS = 2
QUERY_HEADS = 16
NODE_GROUPS = 16
TOTAL_TOKENS = 4096


def paired(key):
    query_unscaled = jax.random.truncated_normal(jax.random.fold_in(key, 11), -4.0, 4.0, (TOTAL_TOKENS, QUERY_HEADS * HEAD_SIZE), jnp.float32)
    key_unscaled = jax.random.truncated_normal(jax.random.fold_in(key, 12), -4.0, 4.0, (TOTAL_TOKENS, KEY_HEADS * HEAD_SIZE), jnp.float32)
    return (query_unscaled, key_unscaled)


def draw_queries(key, part):
    return paired(key)[0].astype(jnp.bfloat16)


def draw_keys(key, part):
    return paired(key)[1].astype(jnp.bfloat16)


def draw_parents(key, part):
    count = NODE_GROUPS
    indices = jnp.arange(count, dtype=jnp.int32)
    order = jax.random.permutation(jax.random.fold_in(key, 21), count).astype(jnp.int32)
    parent_at = jnp.full((count,), -1, jnp.int32)
    depth_at = jnp.zeros((count,), jnp.int32)
    for offset in range(1, count):
        if offset <= MAX_DEPTH:
            chosen = jnp.int32(offset - 1)
        else:
            ranked = jax.random.randint(jax.random.fold_in(key, 100 + offset), (count,), 0, 1 << 20, jnp.int32) * count + indices
            usable = (indices < offset) & (depth_at < MAX_DEPTH)
            chosen = jnp.argmax(jnp.where(usable, ranked, -1)).astype(jnp.int32)
        parent_at = parent_at.at[offset].set(chosen)
        depth_at = depth_at.at[offset].set(depth_at[chosen] + 1)
    mapped = jnp.where(parent_at >= 0, order[jnp.maximum(parent_at, 0)], -1)
    return jnp.zeros((count,), jnp.int32).at[order].set(mapped.astype(jnp.int32))


def steps_of(key, dims, pieces, least, high):
    loudness, own = 1.0, jax.random.fold_in(key, 6)
    for axis_at, blocks in pieces:
        steps = jnp.exp(jax.random.uniform(jax.random.fold_in(own, axis_at), (blocks,), jnp.float32, least / len(pieces), high / len(pieces)))
        loudness = loudness * jnp.repeat(steps, dims[axis_at] // blocks).reshape([-1 if axis == axis_at else 1 for axis in range(len(dims))])
    return loudness


def gaussian(stream_key, extent, deviation, limit, cuts=(), kind=jnp.bfloat16):
    entries = deviation * jax.random.normal(stream_key, extent, jnp.float32)
    if cuts:
        entries = entries * steps_of(stream_key, extent, cuts, -0.22, 0.18)
    return jnp.clip(entries, -limit, limit).astype(kind)


def setup_inputs(seed: int = 0) -> dict:
    seeds = jax.random.split(jax.random.key(seed), 6)
    queries = draw_queries(jax.random.fold_in(seeds[5], 71), 0)
    keys = draw_keys(jax.random.fold_in(seeds[5], 71), 0)
    values = gaussian(seeds[2], (TOTAL_TOKENS, KEY_HEADS * HEAD_SIZE), 1.0, 6.0, ((0, 32),))
    output_gradient = gaussian(seeds[3], (TOTAL_TOKENS, QUERY_HEADS * HEAD_SIZE), 1.0, 6.0, ((0, 16), (1, 2)))
    parents = draw_parents(jax.random.fold_in(seeds[5], 71), 0)
    return dict(queries=queries, keys=keys, values=values, output_gradient=output_gradient, parents=parents)


masked_score = -1e+30

def ancestor_table(parents):
    columns = []
    current = parents
    for level in range(MAX_DEPTH):
        columns.append(current)
        following = parents[jnp.maximum(current, 0)]
        current = jnp.where(current >= 0, following, -1)
    return jnp.stack(columns, axis=1).astype(jnp.int32)

def reference(queries, keys, values, output_gradient, parents):
    scaling = 1.0 / math.sqrt(HEAD_SIZE)
    table = ancestor_table(parents)
    stem_keys = keys.reshape(NODE_GROUPS, NODES_PER_GROUP, NODE_TOKENS, KEY_HEADS, HEAD_SIZE)[:, 0]
    stem_values = values.reshape(NODE_GROUPS, NODES_PER_GROUP, NODE_TOKENS, KEY_HEADS, HEAD_SIZE)[:, 0]
    query_everything = queries.reshape(NODE_GROUPS, NODES_PER_GROUP, NODE_TOKENS, KEY_HEADS, QUERIES_PER_KEY, HEAD_SIZE)
    key_everything = keys.reshape(NODE_GROUPS, NODES_PER_GROUP, NODE_TOKENS, KEY_HEADS, HEAD_SIZE)
    value_everything = values.reshape(NODE_GROUPS, NODES_PER_GROUP, NODE_TOKENS, KEY_HEADS, HEAD_SIZE)
    gradient_total = output_gradient.reshape(NODE_GROUPS, NODES_PER_GROUP, NODE_TOKENS, KEY_HEADS, QUERIES_PER_KEY, HEAD_SIZE)
    positions = jnp.arange(NODE_TOKENS, dtype=jnp.int32)
    causal = positions[:, None] >= positions[None, :]

    def one_group(carried, inputs):
        key_acc, value_acc = carried
        query_group, key_group, value_group, grad_group, slots = inputs
        valid = slots >= 0
        guarded_value = jnp.maximum(slots, 0).astype(jnp.int32)
        selected_keys = stem_keys[guarded_value].reshape(MAX_DEPTH * NODE_TOKENS, KEY_HEADS, HEAD_SIZE)
        selected_values = stem_values[guarded_value].reshape(MAX_DEPTH * NODE_TOKENS, KEY_HEADS, HEAD_SIZE)
        complete_shape = (NODES_PER_GROUP, MAX_DEPTH * NODE_TOKENS, KEY_HEADS, HEAD_SIZE)
        key_cat = jnp.concatenate([jnp.broadcast_to(selected_keys[None], complete_shape), key_group], axis=1).astype(jnp.float32)
        value_cat = jnp.concatenate([jnp.broadcast_to(selected_values[None], complete_shape), value_group], axis=1).astype(jnp.float32)
        ancestor_cols = jnp.repeat(valid, NODE_TOKENS)
        visible = jnp.concatenate([jnp.broadcast_to(ancestor_cols[None, :], (NODE_TOKENS, MAX_DEPTH * NODE_TOKENS)), causal], axis=1)
        query_f = query_group.astype(jnp.float32)
        grad_f = grad_group.astype(jnp.float32)
        scores = jnp.einsum('jrcgd,jkcd->jrcgk', query_f, key_cat) * scaling
        scores = jnp.where(visible[None, :, None, None, :], scores, masked_score)
        peak = lax.optimization_barrier(jnp.max(scores, axis=-1, keepdims=True))
        expo = jnp.exp(scores - peak)
        probs = expo / lax.optimization_barrier(jnp.sum(expo, axis=-1, keepdims=True))
        probs_b = lax.optimization_barrier(probs.astype(jnp.bfloat16)).astype(jnp.float32)
        attended = jnp.einsum('jrcgk,jkcd->jrcgd', probs_b, value_cat).astype(jnp.bfloat16)
        delta = lax.optimization_barrier(jnp.sum(grad_f * attended.astype(jnp.float32), axis=-1))
        dprob = jnp.einsum('jrcgd,jkcd->jrcgk', grad_f, value_cat)
        dscore = probs * (dprob - delta[..., None])
        dscore_b = lax.optimization_barrier(dscore.astype(jnp.bfloat16)).astype(jnp.float32)
        query_gradient = (jnp.einsum('jrcgk,jkcd->jrcgd', dscore_b, key_cat) * scaling).astype(jnp.bfloat16)
        key_columns = jnp.einsum('jrcgk,jrcgd->jkcd', dscore_b, query_f) * scaling
        value_columns = jnp.einsum('jrcgk,jrcgd->jkcd', probs_b, grad_f)
        weight = valid.astype(jnp.float32)[:, None, None, None]
        key_portion = lax.optimization_barrier(jnp.sum(key_columns[:, :MAX_DEPTH * NODE_TOKENS], axis=0)).reshape(MAX_DEPTH, NODE_TOKENS, KEY_HEADS, HEAD_SIZE)
        value_portion = lax.optimization_barrier(jnp.sum(value_columns[:, :MAX_DEPTH * NODE_TOKENS], axis=0)).reshape(MAX_DEPTH, NODE_TOKENS, KEY_HEADS, HEAD_SIZE)
        key_acc = key_acc.at[guarded_value].add(key_portion * weight)
        value_acc = value_acc.at[guarded_value].add(value_portion * weight)
        return ((key_acc, value_acc), (attended, query_gradient, key_columns[:, MAX_DEPTH * NODE_TOKENS:], value_columns[:, MAX_DEPTH * NODE_TOKENS:]))
    begin_offset = (jnp.zeros((NODE_GROUPS, NODE_TOKENS, KEY_HEADS, HEAD_SIZE), jnp.float32), jnp.zeros((NODE_GROUPS, NODE_TOKENS, KEY_HEADS, HEAD_SIZE), jnp.float32))
    (key_acc, value_acc), outputs = lax.scan(one_group, begin_offset, (query_everything, key_everything, value_everything, gradient_total, table))
    attended, query_gradient, key_local, value_local = outputs
    key_local = key_local.at[:, 0].add(key_acc)
    value_local = value_local.at[:, 0].add(value_acc)
    return (attended.reshape(TOTAL_TOKENS, QUERY_HEADS * HEAD_SIZE), query_gradient.reshape(TOTAL_TOKENS, QUERY_HEADS * HEAD_SIZE), key_local.astype(jnp.bfloat16).reshape(TOTAL_TOKENS, KEY_HEADS * HEAD_SIZE), value_local.astype(jnp.bfloat16).reshape(TOTAL_TOKENS, KEY_HEADS * HEAD_SIZE))
```

```python
import functools
import math

import jax
import jax.numpy as jnp
from jax import lax
from jax.experimental import pallas as pl
from jax.experimental.pallas import tpu as pltpu
from jax.sharding import PartitionSpec as P

HEAD_SIZE = 128
NODE_TOKENS = 128
MAX_DEPTH = 6

masked_score = -1e30
TILE_HEADS = 2


def exchange_bits(count):
    bits = []
    bit = count // 2
    while bit:
        bits.append(bit)
        bit //= 2
    return bits


def reverse_bits(value, count):
    result = value * 0
    bit, mirrored = 1, count // 2
    while mirrored:
        result = result + jnp.where((value & bit) != 0, mirrored, 0)
        bit, mirrored = bit * 2, mirrored // 2
    return result


def attention_kernel(
    group_count,
    node_count,
    per_key,
    scaling,
    parents_ref,
    place_ref,
    *refs,
):
    query_refs = refs[:node_count]
    own_refs = refs[node_count : 2 * node_count]
    grad_ref, trunk_ref = refs[2 * node_count : 2 * node_count + 2]
    outs = refs[2 * node_count + 2 :]
    attended_ref = outs[0]
    query_grad_refs = outs[1 : 1 + node_count]
    own_grad_ref, part_ref = outs[1 + node_count : 3 + node_count]
    keys_s, values_s, keys_t, values_t, prob_s, prob_b, score_b, key_acc, value_acc = outs[
        3 + node_count :
    ]
    factor = scaling * math.log2(math.e)
    trunk_rows = MAX_DEPTH * NODE_TOKENS
    total_rows = trunk_rows + NODE_TOKENS
    tile_rows = TILE_HEADS * NODE_TOKENS
    me = place_ref[0]
    current = parents_ref[me]
    spots, valids = [], []
    for level in range(MAX_DEPTH):
        valids.append(current >= 0)
        guarded = jnp.maximum(current, 0)
        spots.append(reverse_bits(guarded ^ me, group_count))
        current = jnp.where(current >= 0, parents_ref[guarded], -1)
    penalties = [jnp.where(valid, 0.0, -masked_score).astype(jnp.float32) for valid in valids]
    penalties.append(None)

    def place_block(block, key, value):
        rows = slice(block * NODE_TOKENS, (block + 1) * NODE_TOKENS)
        keys_s[rows, :] = key
        values_s[rows, :] = value
        keys_t[:, rows] = key.T
        values_t[:, rows] = value.T

    for level in range(MAX_DEPTH):
        pair = trunk_ref[spots[level]]
        place_block(level, pair[:NODE_TOKENS], pair[NODE_TOKENS:])
    key_acc[0:trunk_rows] = jnp.zeros((trunk_rows, HEAD_SIZE), jnp.float32)
    value_acc[0:trunk_rows] = jnp.zeros((trunk_rows, HEAD_SIZE), jnp.float32)
    part_ref[...] = jnp.zeros(part_ref.shape, part_ref.dtype)
    positions_k = lax.broadcasted_iota(jnp.int32, (NODE_TOKENS, tile_rows), 0)
    positions_q = lax.broadcasted_iota(jnp.int32, (NODE_TOKENS, tile_rows), 1) % NODE_TOKENS
    causal = positions_k <= positions_q
    contract_minor = (((1,), (1,)), ((), ()))
    plain = (((1,), (0,)), ((), ()))

    def dot(left, right, dims):
        return lax.dot_general(left, right, dims, preferred_element_type=jnp.float32)

    for node in range(node_count):
        own = own_refs[node]
        place_block(MAX_DEPTH, own[:NODE_TOKENS, :], own[NODE_TOKENS:, :])
        key_acc[trunk_rows:total_rows] = jnp.zeros((NODE_TOKENS, HEAD_SIZE), jnp.float32)
        value_acc[trunk_rows:total_rows] = jnp.zeros((NODE_TOKENS, HEAD_SIZE), jnp.float32)
        query_ref = query_refs[node]
        query_grad_ref = query_grad_refs[node]
        first_column = place_ref[2 + 2 * node]
        grad_rows = pl.ds(
            pl.multiple_of(place_ref[1 + 2 * node] * NODE_TOKENS, NODE_TOKENS), NODE_TOKENS
        )

        def tile(step, carry):
            def columns(offset, index):
                return pl.ds(
                    pl.multiple_of(
                        offset + (step * TILE_HEADS + index) * HEAD_SIZE, HEAD_SIZE
                    ),
                    HEAD_SIZE,
                )

            query = jnp.concatenate(
                [query_ref[:, columns(first_column, i)] for i in range(TILE_HEADS)], axis=0
            )
            grad_pieces = [grad_ref[grad_rows, columns(0, i)] for i in range(TILE_HEADS)]
            grad = jnp.concatenate(grad_pieces, axis=0)
            grad_t = jnp.concatenate([piece.T for piece in grad_pieces], axis=1)
            blocks = [
                slice(b * NODE_TOKENS, (b + 1) * NODE_TOKENS) for b in range(MAX_DEPTH + 1)
            ]
            top = None
            for b, rows in enumerate(blocks):
                scores = dot(keys_s[rows, :], query, contract_minor)
                if penalties[b] is None:
                    scores = jnp.where(causal, scores, masked_score)
                prob_s[rows, :] = scores
                peak = jnp.max(scores, axis=0, keepdims=True)
                if penalties[b] is not None:
                    peak = peak - penalties[b]
                top = peak if top is None else jnp.maximum(top, peak)
            weight_sum = None
            for b, rows in enumerate(blocks):
                shift = top if penalties[b] is None else top + penalties[b]
                weight = jnp.exp2((prob_s[rows, :] - shift) * factor)
                prob_s[rows, :] = weight
                addition = jnp.sum(weight, axis=0, keepdims=True)
                weight_sum = addition if weight_sum is None else weight_sum + addition
            inverse = 1.0 / weight_sum
            for rows in blocks:
                probs = prob_s[rows, :] * inverse
                prob_s[rows, :] = probs
                prob_b[rows, :] = probs.astype(jnp.bfloat16)
            attended = dot(values_t[...], prob_b[...], plain).astype(jnp.bfloat16)
            delta = jnp.sum(
                attended.astype(jnp.float32) * grad_t.astype(jnp.float32), axis=0, keepdims=True
            )
            for rows in blocks:
                prob_grad = dot(values_s[rows, :], grad, contract_minor)
                score_b[rows, :] = (prob_s[rows, :] * (prob_grad - delta)).astype(jnp.bfloat16)
            query_grad = (dot(keys_t[...], score_b[...], plain) * scaling).astype(jnp.bfloat16)
            key_acc[...] += dot(score_b[...], query, plain)
            value_acc[...] += dot(prob_b[...], grad, plain)
            for i in range(TILE_HEADS):
                lanes = slice(i * NODE_TOKENS, (i + 1) * NODE_TOKENS)
                attended_ref[grad_rows, columns(0, i)] = attended[:, lanes].T
                query_grad_ref[:, columns(0, i)] = query_grad[:, lanes].T
            return carry

        lax.fori_loop(0, per_key // TILE_HEADS, tile, 0)
        own_grad_ref[node, :NODE_TOKENS, :] = key_acc[trunk_rows:total_rows] * scaling
        own_grad_ref[node, NODE_TOKENS:, :] = value_acc[trunk_rows:total_rows]

    for level in range(MAX_DEPTH):
        rows = slice(level * NODE_TOKENS, (level + 1) * NODE_TOKENS)

        @pl.when(valids[level])
        def store():
            part_ref[spots[level], :NODE_TOKENS, :] = (key_acc[rows] * scaling).astype(
                part_ref.dtype
            )
            part_ref[spots[level], NODE_TOKENS:, :] = value_acc[rows].astype(part_ref.dtype)


def attention(parents, place, queries, owns, grad, trunks, per_key, scaling):
    node_count = len(queries)
    group_count = trunks.shape[0]
    width = per_key * HEAD_SIZE
    total_rows = (MAX_DEPTH + 1) * NODE_TOKENS
    tile_rows = TILE_HEADS * NODE_TOKENS
    bf16, f32 = jnp.bfloat16, jnp.float32
    smem = pl.BlockSpec(memory_space=pltpu.SMEM)
    vmem = pl.BlockSpec(memory_space=pltpu.VMEM)
    out_shape = (
        [jax.ShapeDtypeStruct((node_count * NODE_TOKENS, width), bf16)]
        + [jax.ShapeDtypeStruct((NODE_TOKENS, width), bf16)] * node_count
        + [jax.ShapeDtypeStruct((node_count, 2 * NODE_TOKENS, HEAD_SIZE), f32)]
        + [jax.ShapeDtypeStruct((group_count, 2 * NODE_TOKENS, HEAD_SIZE), bf16)]
    )
    pairs = node_count * per_key * NODE_TOKENS * total_rows
    results = pl.pallas_call(
        functools.partial(attention_kernel, group_count, node_count, per_key, scaling),
        out_shape=out_shape,
        in_specs=[smem, smem] + [vmem] * (2 * node_count + 2),
        out_specs=[vmem] * len(out_shape),
        scratch_shapes=[
            pltpu.VMEM((total_rows, HEAD_SIZE), bf16),
            pltpu.VMEM((total_rows, HEAD_SIZE), bf16),
            pltpu.VMEM((HEAD_SIZE, total_rows), bf16),
            pltpu.VMEM((HEAD_SIZE, total_rows), bf16),
            pltpu.VMEM((total_rows, tile_rows), f32),
            pltpu.VMEM((total_rows, tile_rows), bf16),
            pltpu.VMEM((total_rows, tile_rows), bf16),
            pltpu.VMEM((total_rows, HEAD_SIZE), f32),
            pltpu.VMEM((total_rows, HEAD_SIZE), f32),
        ],
        cost_estimate=pl.CostEstimate(
            flops=12 * pairs * HEAD_SIZE, transcendentals=pairs, bytes_accessed=8 * 2**20
        ),
    )(parents, place, *queries, *owns, grad, trunks)
    attended = results[0]
    query_grads = results[1 : 1 + node_count]
    own_grads, parts = results[1 + node_count :]
    return attended, query_grads, own_grads, parts


def gather_trunks(trunk, group_count):
    held = trunk[None]
    for bit in exchange_bits(group_count):
        pairs = [(i, i ^ bit) for i in range(group_count)]
        held = jnp.concatenate([held, lax.ppermute(held, "leaf", pairs)], axis=0)
    return held


def scatter_parts(parts, group_count):
    held = parts
    for bit in reversed(exchange_bits(group_count)):
        pairs = [(i, i ^ bit) for i in range(group_count)]
        half = held.shape[0] // 2
        arrived = lax.ppermute(held[half:], "leaf", pairs)
        total = held[:half].astype(jnp.float32) + arrived.astype(jnp.float32)
        held = total if half == 1 else total.astype(jnp.bfloat16)
    return held[0]


def per_device(queries, keys, values, output_gradient, parents):
    head_devices = lax.axis_size("head")
    group_count = lax.axis_size("leaf")
    my_head = lax.axis_index("head")
    my_group = lax.axis_index("leaf").astype(jnp.int32)
    row_count = output_gradient.shape[0]
    node_count = row_count // NODE_TOKENS
    width = output_gradient.shape[1]
    per_key = queries.shape[1] // keys.shape[1]
    scaling = 1.0 / math.sqrt(HEAD_SIZE)
    paired = head_devices == 2 and node_count == 2
    if paired:
        other = 1 - my_head
        swap = [(0, 1), (1, 0)]

        def both(array):
            return array[:, :HEAD_SIZE], array[:, HEAD_SIZE:]

        (key0, key1), (value0, value1) = both(keys), both(values)
        pair0 = jnp.concatenate([key0, value0], axis=0)
        pair1 = jnp.concatenate([key1, value1], axis=0)
        first = my_head == 0
        kept = jnp.where(first, pair0, pair1)
        came = lax.ppermute(jnp.where(first, pair1, pair0), "head", swap)
        trunk = jnp.where(first, kept, came)
        query_send = lax.dynamic_slice_in_dim(queries, other * width, width, 1)
        query_nodes = [queries, lax.ppermute(query_send, "head", swap)]
        owns = [kept, came]
        place = jnp.stack([my_group, my_head, my_head * width, other, other * 0])
    else:
        whole = [
            lax.all_to_all(a, "head", split_axis=1, concat_axis=0, tiled=True)
            for a in (queries, keys, values)
        ]
        starts = [node * NODE_TOKENS for node in range(node_count)]
        query_nodes = [whole[0][s : s + NODE_TOKENS] for s in starts]
        owns = [
            jnp.concatenate([whole[1][s : s + NODE_TOKENS], whole[2][s : s + NODE_TOKENS]], axis=0)
            for s in starts
        ]
        trunk = owns[0]
        place = [my_group]
        for node in range(node_count):
            place += [my_group * 0 + node, my_group * 0]
        place = jnp.stack(place)
    trunks = gather_trunks(trunk, group_count)
    attended, query_grads, own_grads, parts = attention(
        parents, place.astype(jnp.int32), query_nodes, owns, output_gradient, trunks, per_key, scaling
    )
    if paired:
        query_came = lax.ppermute(query_grads[1], "head", swap)
        query_home = jnp.concatenate(
            [
                jnp.where(first, query_grads[0], query_came),
                jnp.where(first, query_came, query_grads[0]),
            ],
            axis=1,
        )
        total = scatter_parts(parts, group_count)
        mine = (own_grads[0] + jnp.where(first, total, 0.0)).astype(jnp.bfloat16)
        theirs = (own_grads[1] + jnp.where(first, 0.0, total)).astype(jnp.bfloat16)
        came_back = lax.ppermute(theirs, "head", swap)
        left = jnp.where(first, mine, came_back)
        right = jnp.where(first, came_back, mine)
        key_home = jnp.concatenate([left[:NODE_TOKENS], right[:NODE_TOKENS]], axis=1)
        value_home = jnp.concatenate([left[NODE_TOKENS:], right[NODE_TOKENS:]], axis=1)
    else:
        total = scatter_parts(parts, group_count)
        grads = [own_grads[0] + total] + [own_grads[node] for node in range(1, node_count)]
        key_grad = jnp.concatenate([g[:NODE_TOKENS] for g in grads], axis=0).astype(jnp.bfloat16)
        value_grad = jnp.concatenate([g[NODE_TOKENS:] for g in grads], axis=0).astype(jnp.bfloat16)
        query_gradient = jnp.concatenate(query_grads, axis=0)
        query_home, key_home, value_home = [
            lax.all_to_all(a, "head", split_axis=0, concat_axis=1, tiled=True)
            for a in (query_gradient, key_grad, value_grad)
        ]
    return (attended, query_home, key_home, value_home)


def solution(mesh):
    placed = (
        P(("leaf", "head"), None),
        P(("leaf", "head"), None),
        P(("leaf", "head"), None),
        P("leaf", "head"),
        P(),
    )
    return jax.shard_map(
        per_device,
        mesh=mesh,
        in_specs=placed,
        out_specs=(
            P("leaf", "head"),
            P(("leaf", "head"), None),
            P(("leaf", "head"), None),
            P(("leaf", "head"), None),
        ),
        check_vma=False,
    )
```

```python
import functools
import math

import jax
import jax.numpy as jnp
from jax import lax
from jax.experimental import pallas as pl
from jax.experimental.pallas import tpu as pltpu
from jax.sharding import PartitionSpec as P


HEAD_SIZE = 128
NODE_TOKENS = 128
MAX_DEPTH = 6

masked_score = -1e30
TILE_HEADS = 2


def exchange_bits(count):
    bits = []
    bit = count // 2
    while bit:
        bits.append(bit)
        bit //= 2
    return bits


def reverse_bits(value, count):
    result = value * 0
    bit, mirrored = 1, count // 2
    while mirrored:
        result = result + jnp.where((value & bit) != 0, mirrored, 0)
        bit, mirrored = bit * 2, mirrored // 2
    return result


def attention_kernel(
    group_count,
    node_count,
    per_key,
    scaling,
    parents_ref,
    place_ref,
    *refs,
):
    query_refs = refs[:node_count]
    own_refs = refs[node_count : 2 * node_count]
    grad_ref, trunk_ref = refs[2 * node_count : 2 * node_count + 2]
    outs = refs[2 * node_count + 2 :]
    attended_ref = outs[0]
    query_grad_refs = outs[1 : 1 + node_count]
    own_grad_ref, near_ref, far_ref = outs[1 + node_count : 4 + node_count]
    keys_s, values_s, keys_t, values_t, weight_f, weight_b, score_b, key_acc, value_acc = outs[
        4 + node_count :
    ]
    factor = scaling * math.log2(math.e)
    trunk_rows = MAX_DEPTH * NODE_TOKENS
    half = group_count // 2
    tile_rows = TILE_HEADS * NODE_TOKENS
    me = place_ref[0]
    current = parents_ref[me]
    spots, valids = [], []
    for _ in range(MAX_DEPTH):
        valids.append(current >= 0)
        guarded = jnp.maximum(current, 0)
        spots.append(reverse_bits(guarded ^ me, group_count))
        current = jnp.where(current >= 0, parents_ref[guarded], -1)
    penalties = [jnp.where(valid, 0.0, -masked_score).astype(jnp.float32) for valid in valids]
    penalties.append(None)
    contract_minor = (((1,), (1,)), ((), ()))
    plain = (((1,), (0,)), ((), ()))

    def dot(left, right, dims):
        return lax.dot_general(left, right, dims, preferred_element_type=jnp.float32)

    def place_block(block, key, value):
        rows = slice(block * NODE_TOKENS, (block + 1) * NODE_TOKENS)
        keys_s[rows, :] = key
        values_s[rows, :] = value
        keys_t[:, rows] = key.T
        values_t[:, rows] = value.T

    for level in range(MAX_DEPTH):
        pair = trunk_ref[spots[level]]
        place_block(level, pair[:NODE_TOKENS], pair[NODE_TOKENS:])
    for node in range(node_count):
        own = own_refs[node]
        place_block(MAX_DEPTH + node, own[:NODE_TOKENS, :], own[NODE_TOKENS:, :])
    positions_k = lax.broadcasted_iota(jnp.int32, (NODE_TOKENS, tile_rows), 0)
    positions_q = lax.broadcasted_iota(jnp.int32, (NODE_TOKENS, tile_rows), 1) % NODE_TOKENS
    causal = positions_k <= positions_q
    started = set()

    def block_rows(block):
        return slice(block * NODE_TOKENS, (block + 1) * NODE_TOKENS)

    class Tile:
        def __init__(self, index, node, first_head):
            self.slot = index % 2
            self.node = node
            self.first_head = first_head
            self.blocks = list(range(MAX_DEPTH)) + [MAX_DEPTH + node]
            self.grad_rows = pl.ds(
                pl.multiple_of(place_ref[1 + 2 * node] * NODE_TOKENS, NODE_TOKENS), NODE_TOKENS
            )

        def columns(self, offset, i):
            start = (self.first_head + i) * HEAD_SIZE
            if offset is None:
                return slice(start, start + HEAD_SIZE)
            return pl.ds(pl.multiple_of(offset + start, HEAD_SIZE), HEAD_SIZE)

        def query(self):
            offset = place_ref[2 + 2 * self.node]
            pieces = [
                query_refs[self.node][:, self.columns(offset, i)] for i in range(TILE_HEADS)
            ]
            return jnp.concatenate(pieces, axis=0)

        def forward(self):
            query = self.query()
            top = None
            for b, block in enumerate(self.blocks):
                scores = dot(keys_s[block_rows(block), :], query, contract_minor)
                if b == MAX_DEPTH:
                    scores = jnp.where(causal, scores, masked_score)
                weight_f[self.slot, block_rows(b), :] = scores
                peak = jnp.max(scores, axis=0, keepdims=True)
                if b < MAX_DEPTH:
                    peak = peak - penalties[b]
                top = peak if top is None else jnp.maximum(top, peak)
                yield
            weight_sum = None
            for b in range(MAX_DEPTH + 1):
                shift = top if b == MAX_DEPTH else top + penalties[b]
                weight = jnp.exp2((weight_f[self.slot, block_rows(b), :] - shift) * factor)
                weight_f[self.slot, block_rows(b), :] = weight
                weight_b[self.slot, block_rows(b), :] = weight.astype(jnp.bfloat16)
                addition = jnp.sum(weight, axis=0, keepdims=True)
                weight_sum = addition if weight_sum is None else weight_sum + addition
                yield
            self.inverse = 1.0 / weight_sum

        def backward(self):
            grad_t = jnp.concatenate(
                [grad_ref[self.grad_rows, self.columns(None, i)].T for i in range(TILE_HEADS)],
                axis=1,
            )
            scaled_t = (grad_t.astype(jnp.float32) * self.inverse).astype(jnp.bfloat16)
            trunk = slice(0, trunk_rows)
            own_block = self.blocks[-1]
            attended = dot(values_t[:, trunk], weight_b[self.slot, trunk, :], plain)
            attended += dot(
                values_t[:, block_rows(own_block)],
                weight_b[self.slot, block_rows(MAX_DEPTH), :],
                plain,
            )
            attended = (attended * self.inverse).astype(jnp.bfloat16)
            delta = jnp.sum(
                attended.astype(jnp.float32) * scaled_t.astype(jnp.float32),
                axis=0,
                keepdims=True,
            )
            for i in range(TILE_HEADS):
                attended_ref[self.grad_rows, self.columns(None, i)] = attended[
                    :, block_rows(i)
                ].T
            yield
            for b, block in enumerate(self.blocks):
                prob_grad = dot(values_s[block_rows(block), :], scaled_t, plain)
                weight = weight_f[self.slot, block_rows(b), :]
                score_b[self.slot, block_rows(b), :] = (weight * (prob_grad - delta)).astype(
                    jnp.bfloat16
                )
                yield
            query = self.query()
            for b, block in enumerate(self.blocks):
                key_part = dot(score_b[self.slot, block_rows(b), :], query, plain)
                value_part = dot(weight_b[self.slot, block_rows(b), :], scaled_t, contract_minor)
                if block in started:
                    key_acc[block_rows(block), :] += key_part
                    value_acc[block_rows(block), :] += value_part
                else:
                    key_acc[block_rows(block), :] = key_part
                    value_acc[block_rows(block), :] = value_part
                    started.add(block)
                yield
            query_grad = dot(keys_t[:, trunk], score_b[self.slot, trunk, :], plain)
            query_grad += dot(
                keys_t[:, block_rows(own_block)],
                score_b[self.slot, block_rows(MAX_DEPTH), :],
                plain,
            )
            query_grad = (query_grad * scaling).astype(jnp.bfloat16)
            for i in range(TILE_HEADS):
                query_grad_refs[self.node][:, self.columns(None, i)] = query_grad[
                    :, block_rows(i)
                ].T
            yield

    tiles = []
    for node in range(node_count):
        for first_head in range(0, per_key, TILE_HEADS):
            tiles.append(Tile(len(tiles), node, first_head))
    before = iter(())
    for tile in tiles + [None]:
        running = [before] + ([tile.forward()] if tile is not None else [])
        while running:
            for stream in list(running):
                if next(stream, running) is running:
                    running.remove(stream)
        before = tile.backward() if tile is not None else iter(())

    for node in range(node_count):
        rows = block_rows(MAX_DEPTH + node)
        own_grad_ref[node, :NODE_TOKENS, :] = key_acc[rows, :] * scaling
        own_grad_ref[node, NODE_TOKENS:, :] = value_acc[rows, :]
    near_ref[...] = jnp.zeros(near_ref.shape, near_ref.dtype)
    far_ref[...] = jnp.zeros(far_ref.shape, far_ref.dtype)
    for level in range(MAX_DEPTH):

        def store(part_ref, spot, rows=block_rows(level)):
            part_ref[spot, :NODE_TOKENS, :] = (key_acc[rows, :] * scaling).astype(part_ref.dtype)
            part_ref[spot, NODE_TOKENS:, :] = value_acc[rows, :].astype(part_ref.dtype)

        spot = spots[level]
        pl.when(valids[level] & (spot < half))(functools.partial(store, near_ref, spot))
        pl.when(valids[level] & (spot >= half))(functools.partial(store, far_ref, spot - half))


def attention(parents, place, queries, owns, grad, trunks, per_key, scaling):
    node_count = len(queries)
    group_count = trunks.shape[0]
    width = per_key * HEAD_SIZE
    block_count = MAX_DEPTH + node_count
    held_rows = block_count * NODE_TOKENS
    seen_rows = (MAX_DEPTH + 1) * NODE_TOKENS
    tile_rows = TILE_HEADS * NODE_TOKENS
    bf16, f32 = jnp.bfloat16, jnp.float32
    smem = pl.BlockSpec(memory_space=pltpu.SMEM)
    vmem = pl.BlockSpec(memory_space=pltpu.VMEM)
    half_shape = jax.ShapeDtypeStruct((group_count // 2, 2 * NODE_TOKENS, HEAD_SIZE), bf16)
    out_shape = (
        [jax.ShapeDtypeStruct((node_count * NODE_TOKENS, width), bf16)]
        + [jax.ShapeDtypeStruct((NODE_TOKENS, width), bf16)] * node_count
        + [jax.ShapeDtypeStruct((node_count, 2 * NODE_TOKENS, HEAD_SIZE), f32)]
        + [half_shape, half_shape]
    )
    pairs = node_count * per_key * NODE_TOKENS * seen_rows
    results = pl.pallas_call(
        functools.partial(attention_kernel, group_count, node_count, per_key, scaling),
        out_shape=out_shape,
        in_specs=[smem, smem] + [vmem] * (2 * node_count + 2),
        out_specs=[vmem] * len(out_shape),
        scratch_shapes=[
            pltpu.VMEM((held_rows, HEAD_SIZE), bf16),
            pltpu.VMEM((held_rows, HEAD_SIZE), bf16),
            pltpu.VMEM((HEAD_SIZE, held_rows), bf16),
            pltpu.VMEM((HEAD_SIZE, held_rows), bf16),
            pltpu.VMEM((2, seen_rows, tile_rows), f32),
            pltpu.VMEM((2, seen_rows, tile_rows), bf16),
            pltpu.VMEM((2, seen_rows, tile_rows), bf16),
            pltpu.VMEM((held_rows, HEAD_SIZE), f32),
            pltpu.VMEM((held_rows, HEAD_SIZE), f32),
        ],
        cost_estimate=pl.CostEstimate(
            flops=12 * pairs * HEAD_SIZE, transcendentals=pairs, bytes_accessed=8 * 2**20
        ),
    )(parents, place, *queries, *owns, grad, trunks)
    attended = results[0]
    query_grads = results[1 : 1 + node_count]
    own_grads = results[1 + node_count]
    parts = results[2 + node_count :]
    return attended, query_grads, own_grads, parts


def partner_pairs(count, bit):
    return [(i, i ^ bit) for i in range(count)]


def widen_trunks(held, bits, group_count):
    for bit in bits:
        arrived = lax.ppermute(held, "leaf", partner_pairs(group_count, bit))
        held = jnp.concatenate([held, arrived], axis=0)
    return held


def narrow_parts(near, far, bits, group_count):
    for bit in bits:
        arrived = lax.ppermute(far, "leaf", partner_pairs(group_count, bit))
        total = near.astype(jnp.float32) + arrived.astype(jnp.float32)
        half = near.shape[0] // 2
        total = total.astype(jnp.bfloat16)
        near, far = total[:half], total[half:]
    return near, far


def pair_of(arrays, columns):
    return jnp.concatenate([array[:, columns] for array in arrays], axis=0)


def paired_device(queries, keys, values, output_gradient, parents, per_key, scaling):
    group_count = lax.axis_size("leaf")
    my_head = lax.axis_index("head")
    my_group = lax.axis_index("leaf").astype(jnp.int32)
    width = output_gradient.shape[1]
    swap = [(0, 1), (1, 0)]
    bits = exchange_bits(group_count)
    far_bit = bits[0]
    both = ("leaf", "head")
    straight = [(2 * g, 2 * (g ^ far_bit)) for g in range(group_count)]
    across = [(2 * g, 2 * (g ^ far_bit) + 1) for g in range(group_count)]
    gathered = [(2 * g + 1, 2 * (g ^ far_bit)) for g in range(group_count)]
    first = my_head == 0
    other = 1 - my_head
    pair0 = pair_of((keys, values), slice(0, HEAD_SIZE))
    pair1 = pair_of((keys, values), slice(HEAD_SIZE, 2 * HEAD_SIZE))
    kept = jnp.where(first, pair0, pair1)
    came = lax.ppermute(jnp.where(first, pair1, pair0), "head", swap)
    far0 = lax.ppermute(pair0, both, straight)
    far1 = lax.ppermute(pair1, both, across)
    query_send = lax.dynamic_slice_in_dim(queries, other * width, width, 1)
    query_came = lax.ppermute(query_send, "head", swap)
    held = jnp.stack([jnp.where(first, kept, came), jnp.where(first, far0, far1)])
    trunks = widen_trunks(held, bits[1:], group_count)
    place = jnp.stack([my_group, my_head, my_head * width, other, other * 0]).astype(jnp.int32)
    attended, query_grads, own_grads, (near, far) = attention(
        parents,
        place,
        [queries, query_came],
        [kept, came],
        output_gradient,
        trunks,
        per_key,
        scaling,
    )
    near, far = narrow_parts(near, far, bits[:0:-1], group_count)
    query_back = lax.ppermute(query_grads[1], "head", swap)
    near, far = near[0].astype(jnp.float32), far[0]
    nothing = jnp.zeros_like(near)
    theirs = (own_grads[1] + jnp.where(first, nothing, near)).astype(jnp.bfloat16)
    far1 = lax.ppermute(far, both, gathered)
    came_back = lax.ppermute(theirs, "head", swap)
    far0 = lax.ppermute(far, both, straight)
    f32 = jnp.float32
    mine = own_grads[0] + jnp.where(first, near + far0.astype(f32), nothing)
    cross = came_back.astype(f32) + jnp.where(first, far1.astype(f32), nothing)
    left = jnp.where(first, mine, cross).astype(jnp.bfloat16)
    right = jnp.where(first, cross, mine).astype(jnp.bfloat16)
    key_home = jnp.concatenate([left[:NODE_TOKENS], right[:NODE_TOKENS]], axis=1)
    value_home = jnp.concatenate([left[NODE_TOKENS:], right[NODE_TOKENS:]], axis=1)
    query_home = jnp.concatenate(
        [
            jnp.where(first, query_grads[0], query_back),
            jnp.where(first, query_back, query_grads[0]),
        ],
        axis=1,
    )
    return (attended, query_home, key_home, value_home)


def general_device(queries, keys, values, output_gradient, parents, per_key, scaling):
    group_count = lax.axis_size("leaf")
    my_group = lax.axis_index("leaf").astype(jnp.int32)
    node_count = output_gradient.shape[0] // NODE_TOKENS
    bits = exchange_bits(group_count)
    query_all, key_all, value_all = [
        lax.all_to_all(a, "head", split_axis=1, concat_axis=0, tiled=True)
        for a in (queries, keys, values)
    ]
    spans = [slice(n * NODE_TOKENS, (n + 1) * NODE_TOKENS) for n in range(node_count)]
    owns = [jnp.concatenate([key_all[s], value_all[s]], axis=0) for s in spans]
    trunks = widen_trunks(owns[0][None], bits, group_count)
    zero = my_group * 0
    place = [my_group]
    for node in range(node_count):
        place += [zero + node, zero]
    attended, query_grads, own_grads, (near, far) = attention(
        parents,
        jnp.stack(place),
        [query_all[s] for s in spans],
        owns,
        output_gradient,
        trunks,
        per_key,
        scaling,
    )
    near, far = narrow_parts(near, far, bits[:0:-1], group_count)
    arrived = lax.ppermute(far, "leaf", partner_pairs(group_count, bits[0]))
    total = near[0].astype(jnp.float32) + arrived[0].astype(jnp.float32)
    grads = [own_grads[0] + total] + [own_grads[node] for node in range(1, node_count)]
    key_grad = jnp.concatenate([g[:NODE_TOKENS] for g in grads], axis=0).astype(jnp.bfloat16)
    value_grad = jnp.concatenate([g[NODE_TOKENS:] for g in grads], axis=0).astype(jnp.bfloat16)
    query_gradient = jnp.concatenate(query_grads, axis=0)
    query_home, key_home, value_home = [
        lax.all_to_all(a, "head", split_axis=0, concat_axis=1, tiled=True)
        for a in (query_gradient, key_grad, value_grad)
    ]
    return (attended, query_home, key_home, value_home)


def per_device(queries, keys, values, output_gradient, parents):
    node_count = output_gradient.shape[0] // NODE_TOKENS
    per_key = queries.shape[1] // keys.shape[1]
    scaling = 1.0 / math.sqrt(HEAD_SIZE)
    paired = lax.axis_size("head") == 2 and node_count == 2
    body = paired_device if paired else general_device
    return body(queries, keys, values, output_gradient, parents, per_key, scaling)


def solution(mesh):
    placed = (
        P(("leaf", "head"), None),
        P(("leaf", "head"), None),
        P(("leaf", "head"), None),
        P("leaf", "head"),
        P(),
    )
    return jax.shard_map(
        per_device,
        mesh=mesh,
        in_specs=placed,
        out_specs=(
            P("leaf", "head"),
            P(("leaf", "head"), None),
            P(("leaf", "head"), None),
            P(("leaf", "head"), None),
        ),
        check_vma=False,
    )
```

```python
import functools
import math

import jax
import jax.numpy as jnp
from jax import lax
from jax.experimental import pallas as pl
from jax.experimental.pallas import tpu as pltpu
from jax.sharding import PartitionSpec as P


HEAD_SIZE = 128
NODE_TOKENS = 128
MAX_DEPTH = 6

masked_score = -1e30
TILE_HEADS = 2
KERNEL_BYTES = 24 * 2**20


def exchange_bits(count):
    bits = []
    bit = count // 2
    while bit:
        bits.append(bit)
        bit //= 2
    return bits


def reverse_bits(value, count):
    result = value * 0
    bit, mirrored = 1, count // 2
    while mirrored:
        result = result + jnp.where((value & bit) != 0, mirrored, 0)
        bit, mirrored = bit * 2, mirrored // 2
    return result


def ring_size(group_count):
    return 4 if group_count % 4 == 0 else 1


def relative_spots(me, target, group_count):
    ring = ring_size(group_count)
    inner = group_count // ring
    me_ring, target_ring = me // inner, target // inner
    block = ring * reverse_bits((me % inner) ^ (target % inner), inner)
    gathered = block + (me_ring - target_ring + ring) % ring
    returned = block + (target_ring - me_ring + ring) % ring
    return gathered, returned


def attention_kernel(
    group_count,
    node_count,
    per_key,
    scaling,
    parents_ref,
    place_ref,
    *refs,
):
    query_refs = refs[:node_count]
    own_refs = refs[node_count : 2 * node_count]
    grad_ref, trunk_ref = refs[2 * node_count : 2 * node_count + 2]
    outs = refs[2 * node_count + 2 :]
    attended_ref = outs[0]
    query_grad_refs = outs[1 : 1 + node_count]
    own_grad_ref, near_ref, far_ref = outs[1 + node_count : 4 + node_count]
    keys_s, values_s, keys_t, values_t, weight_f, weight_b, score_b, key_acc, value_acc = outs[
        4 + node_count :
    ]
    factor = scaling * math.log2(math.e)
    trunk_rows = MAX_DEPTH * NODE_TOKENS
    half = group_count // 2
    tile_rows = TILE_HEADS * NODE_TOKENS
    me = place_ref[0]
    current = parents_ref[me]
    spots, back_spots, valids = [], [], []
    for _ in range(MAX_DEPTH):
        valids.append(current >= 0)
        guarded = jnp.maximum(current, 0)
        gathered, returned = relative_spots(me, guarded, group_count)
        spots.append(gathered)
        back_spots.append(returned)
        current = jnp.where(current >= 0, parents_ref[guarded], -1)
    penalties = [jnp.where(valid, 0.0, -masked_score).astype(jnp.float32) for valid in valids]
    penalties.append(None)
    contract_minor = (((1,), (1,)), ((), ()))
    plain = (((1,), (0,)), ((), ()))

    def dot(left, right, dims):
        return lax.dot_general(left, right, dims, preferred_element_type=jnp.float32)

    def place_block(block, key, value):
        rows = slice(block * NODE_TOKENS, (block + 1) * NODE_TOKENS)
        keys_s[rows, :] = key
        values_s[rows, :] = value
        keys_t[:, rows] = key.T
        values_t[:, rows] = value.T

    for level in range(MAX_DEPTH):
        pair = trunk_ref[spots[level]]
        place_block(level, pair[:NODE_TOKENS], pair[NODE_TOKENS:])
    for node in range(node_count):
        own = own_refs[node]
        place_block(MAX_DEPTH + node, own[:NODE_TOKENS, :], own[NODE_TOKENS:, :])
    positions_k = lax.broadcasted_iota(jnp.int32, (NODE_TOKENS, tile_rows), 0)
    positions_q = lax.broadcasted_iota(jnp.int32, (NODE_TOKENS, tile_rows), 1) % NODE_TOKENS
    causal = positions_k <= positions_q
    started = set()

    def block_rows(block):
        return slice(block * NODE_TOKENS, (block + 1) * NODE_TOKENS)

    class Tile:
        def __init__(self, index, node, first_head):
            self.slot = index % 2
            self.node = node
            self.first_head = first_head
            self.blocks = list(range(MAX_DEPTH)) + [MAX_DEPTH + node]
            self.grad_rows = pl.ds(
                pl.multiple_of(place_ref[1 + 2 * node] * NODE_TOKENS, NODE_TOKENS), NODE_TOKENS
            )

        def columns(self, offset, i):
            start = (self.first_head + i) * HEAD_SIZE
            if offset is None:
                return slice(start, start + HEAD_SIZE)
            return pl.ds(pl.multiple_of(offset + start, HEAD_SIZE), HEAD_SIZE)

        def query(self):
            offset = place_ref[2 + 2 * self.node]
            pieces = [
                query_refs[self.node][:, self.columns(offset, i)] for i in range(TILE_HEADS)
            ]
            return jnp.concatenate(pieces, axis=0)

        def forward(self):
            query = self.query()
            top = None
            for b, block in enumerate(self.blocks):
                scores = dot(keys_s[block_rows(block), :], query, contract_minor)
                if b == MAX_DEPTH:
                    scores = jnp.where(causal, scores, masked_score)
                weight_f[self.slot, block_rows(b), :] = scores
                peak = jnp.max(scores, axis=0, keepdims=True)
                if b < MAX_DEPTH:
                    peak = peak - penalties[b]
                top = peak if top is None else jnp.maximum(top, peak)
                yield
            weight_sum = None
            for b in range(MAX_DEPTH + 1):
                shift = top if b == MAX_DEPTH else top + penalties[b]
                weight = jnp.exp2((weight_f[self.slot, block_rows(b), :] - shift) * factor)
                weight_f[self.slot, block_rows(b), :] = weight
                weight_b[self.slot, block_rows(b), :] = weight.astype(jnp.bfloat16)
                addition = jnp.sum(weight, axis=0, keepdims=True)
                weight_sum = addition if weight_sum is None else weight_sum + addition
                yield
            self.inverse = 1.0 / weight_sum

        def backward(self):
            grad_t = jnp.concatenate(
                [grad_ref[self.grad_rows, self.columns(None, i)].T for i in range(TILE_HEADS)],
                axis=1,
            )
            scaled_t = (grad_t.astype(jnp.float32) * self.inverse).astype(jnp.bfloat16)
            trunk = slice(0, trunk_rows)
            own_block = self.blocks[-1]
            attended = dot(values_t[:, trunk], weight_b[self.slot, trunk, :], plain)
            attended += dot(
                values_t[:, block_rows(own_block)],
                weight_b[self.slot, block_rows(MAX_DEPTH), :],
                plain,
            )
            attended = (attended * self.inverse).astype(jnp.bfloat16)
            delta = jnp.sum(
                attended.astype(jnp.float32) * scaled_t.astype(jnp.float32),
                axis=0,
                keepdims=True,
            )
            for i in range(TILE_HEADS):
                attended_ref[self.grad_rows, self.columns(None, i)] = attended[
                    :, block_rows(i)
                ].T
            yield
            for b, block in enumerate(self.blocks):
                prob_grad = dot(values_s[block_rows(block), :], scaled_t, plain)
                weight = weight_f[self.slot, block_rows(b), :]
                score_b[self.slot, block_rows(b), :] = (weight * (prob_grad - delta)).astype(
                    jnp.bfloat16
                )
                yield
            query = self.query()
            for b, block in enumerate(self.blocks):
                key_part = dot(score_b[self.slot, block_rows(b), :], query, plain)
                value_part = dot(weight_b[self.slot, block_rows(b), :], scaled_t, contract_minor)
                if block in started:
                    key_acc[block_rows(block), :] += key_part
                    value_acc[block_rows(block), :] += value_part
                else:
                    key_acc[block_rows(block), :] = key_part
                    value_acc[block_rows(block), :] = value_part
                    started.add(block)
                yield
            query_grad = dot(keys_t[:, trunk], score_b[self.slot, trunk, :], plain)
            query_grad += dot(
                keys_t[:, block_rows(own_block)],
                score_b[self.slot, block_rows(MAX_DEPTH), :],
                plain,
            )
            query_grad = (query_grad * scaling).astype(jnp.bfloat16)
            for i in range(TILE_HEADS):
                query_grad_refs[self.node][:, self.columns(None, i)] = query_grad[
                    :, block_rows(i)
                ].T
            yield

    tiles = []
    for node in range(node_count):
        for first_head in range(0, per_key, TILE_HEADS):
            tiles.append(Tile(len(tiles), node, first_head))
    before = iter(())
    for tile in tiles + [None]:
        running = [before] + ([tile.forward()] if tile is not None else [])
        while running:
            for stream in list(running):
                if next(stream, running) is running:
                    running.remove(stream)
        before = tile.backward() if tile is not None else iter(())

    for node in range(node_count):
        rows = block_rows(MAX_DEPTH + node)
        own_grad_ref[node, :NODE_TOKENS, :] = key_acc[rows, :] * scaling
        own_grad_ref[node, NODE_TOKENS:, :] = value_acc[rows, :]
    near_ref[...] = jnp.zeros(near_ref.shape, near_ref.dtype)
    far_ref[...] = jnp.zeros(far_ref.shape, far_ref.dtype)
    for level in range(MAX_DEPTH):

        def store(part_ref, spot, rows=block_rows(level)):
            part_ref[spot, :NODE_TOKENS, :] = (key_acc[rows, :] * scaling).astype(part_ref.dtype)
            part_ref[spot, NODE_TOKENS:, :] = value_acc[rows, :].astype(part_ref.dtype)

        spot = back_spots[level]
        pl.when(valids[level] & (spot < half))(functools.partial(store, near_ref, spot))
        pl.when(valids[level] & (spot >= half))(functools.partial(store, far_ref, spot - half))


def on_chip(array):
    return pltpu.with_memory_space_constraint(array, pltpu.VMEM)


def attention(parents, place, queries, owns, grad, trunks, per_key, scaling):
    node_count = len(queries)
    group_count = trunks.shape[0]
    width = per_key * HEAD_SIZE
    block_count = MAX_DEPTH + node_count
    held_rows = block_count * NODE_TOKENS
    seen_rows = (MAX_DEPTH + 1) * NODE_TOKENS
    tile_rows = TILE_HEADS * NODE_TOKENS
    bf16, f32 = jnp.bfloat16, jnp.float32
    smem = pl.BlockSpec(memory_space=pltpu.SMEM)
    vmem = pl.BlockSpec(memory_space=pltpu.VMEM)
    half_shape = pltpu.VMEM((group_count // 2, 2 * NODE_TOKENS, HEAD_SIZE), bf16)
    out_shape = (
        [pltpu.VMEM((node_count * NODE_TOKENS, width), bf16)]
        + [pltpu.VMEM((NODE_TOKENS, width), bf16)] * node_count
        + [pltpu.VMEM((node_count, 2 * NODE_TOKENS, HEAD_SIZE), f32)]
        + [half_shape, half_shape]
    )
    pairs = node_count * per_key * NODE_TOKENS * seen_rows
    results = pl.pallas_call(
        functools.partial(attention_kernel, group_count, node_count, per_key, scaling),
        out_shape=out_shape,
        in_specs=[smem, smem] + [vmem] * (2 * node_count + 2),
        out_specs=[vmem] * len(out_shape),
        scratch_shapes=[
            pltpu.VMEM((held_rows, HEAD_SIZE), bf16),
            pltpu.VMEM((held_rows, HEAD_SIZE), bf16),
            pltpu.VMEM((HEAD_SIZE, held_rows), bf16),
            pltpu.VMEM((HEAD_SIZE, held_rows), bf16),
            pltpu.VMEM((2, seen_rows, tile_rows), f32),
            pltpu.VMEM((2, seen_rows, tile_rows), bf16),
            pltpu.VMEM((2, seen_rows, tile_rows), bf16),
            pltpu.VMEM((held_rows, HEAD_SIZE), f32),
            pltpu.VMEM((held_rows, HEAD_SIZE), f32),
        ],
        compiler_params=pltpu.CompilerParams(vmem_limit_bytes=KERNEL_BYTES),
        cost_estimate=pl.CostEstimate(
            flops=12 * pairs * HEAD_SIZE, transcendentals=pairs, bytes_accessed=8 * 2**20
        ),
    )(
        parents,
        place,
        *[on_chip(a) for a in (*queries, *owns, grad, trunks)],
    )
    attended = results[0]
    query_grads = results[1 : 1 + node_count]
    own_grads = results[1 + node_count]
    parts = results[2 + node_count :]
    return attended, query_grads, own_grads, parts


def partner_pairs(count, bit):
    return [(i, i ^ bit) for i in range(count)]


def ring_pairs(count, shift):
    ring = ring_size(count)
    inner = count // ring
    return [(i, (i // inner + shift) % ring * inner + i % inner) for i in range(count)]


def gather_trunks(trunk, group_count):
    ring = ring_size(group_count)
    pieces = [trunk]
    for shift in range(1, ring):
        pieces.append(lax.ppermute(trunk, "leaf", ring_pairs(group_count, shift)))
    held = jnp.stack(pieces)
    for bit in exchange_bits(group_count // ring):
        arrived = lax.ppermute(held, "leaf", partner_pairs(group_count, bit))
        held = jnp.concatenate([held, arrived], axis=0)
    return held


def return_parts(near, far, group_count):
    ring = ring_size(group_count)
    for bit in reversed(exchange_bits(group_count // ring)):
        arrived = lax.ppermute(far, "leaf", partner_pairs(group_count, bit))
        total = near.astype(jnp.float32) + arrived.astype(jnp.float32)
        total = total.astype(jnp.bfloat16)
        half = near.shape[0] // 2
        near, far = (total[:half], total[half:]) if half >= ring else (total, None)
    total = near[0].astype(jnp.float32)
    for shift in range(1, ring):
        arrived = lax.ppermute(near[shift], "leaf", ring_pairs(group_count, shift))
        total = total + arrived.astype(jnp.float32)
    return total


def pair_of(arrays, columns):
    return jnp.concatenate([array[:, columns] for array in arrays], axis=0)


def paired_device(queries, keys, values, output_gradient, parents, per_key, scaling):
    group_count = lax.axis_size("leaf")
    my_head = lax.axis_index("head")
    my_group = lax.axis_index("leaf").astype(jnp.int32)
    width = output_gradient.shape[1]
    swap = [(0, 1), (1, 0)]
    first = my_head == 0
    other = 1 - my_head
    pair0 = pair_of((keys, values), slice(0, HEAD_SIZE))
    pair1 = pair_of((keys, values), slice(HEAD_SIZE, 2 * HEAD_SIZE))
    kept = jnp.where(first, pair0, pair1)
    came = lax.ppermute(jnp.where(first, pair1, pair0), "head", swap)
    query_send = lax.dynamic_slice_in_dim(queries, other * width, width, 1)
    query_came = lax.ppermute(query_send, "head", swap)
    trunks = gather_trunks(jnp.where(first, kept, came), group_count)
    place = jnp.stack([my_group, my_head, my_head * width, other, other * 0]).astype(jnp.int32)
    attended, query_grads, own_grads, (near, far) = attention(
        parents,
        place,
        [queries, query_came],
        [kept, came],
        output_gradient,
        trunks,
        per_key,
        scaling,
    )
    query_back = lax.ppermute(query_grads[1], "head", swap)
    total = return_parts(near, far, group_count)
    nothing = jnp.zeros_like(total)
    mine = (own_grads[0] + jnp.where(first, total, nothing)).astype(jnp.bfloat16)
    theirs = (own_grads[1] + jnp.where(first, nothing, total)).astype(jnp.bfloat16)
    came_back = lax.ppermute(theirs, "head", swap)
    left = jnp.where(first, mine, came_back)
    right = jnp.where(first, came_back, mine)
    key_home = jnp.concatenate([left[:NODE_TOKENS], right[:NODE_TOKENS]], axis=1)
    value_home = jnp.concatenate([left[NODE_TOKENS:], right[NODE_TOKENS:]], axis=1)
    query_home = jnp.concatenate(
        [
            jnp.where(first, query_grads[0], query_back),
            jnp.where(first, query_back, query_grads[0]),
        ],
        axis=1,
    )
    return (attended, query_home, key_home, value_home)


def general_device(queries, keys, values, output_gradient, parents, per_key, scaling):
    group_count = lax.axis_size("leaf")
    my_group = lax.axis_index("leaf").astype(jnp.int32)
    node_count = output_gradient.shape[0] // NODE_TOKENS
    query_all, key_all, value_all = [
        lax.all_to_all(a, "head", split_axis=1, concat_axis=0, tiled=True)
        for a in (queries, keys, values)
    ]
    spans = [slice(n * NODE_TOKENS, (n + 1) * NODE_TOKENS) for n in range(node_count)]
    owns = [jnp.concatenate([key_all[s], value_all[s]], axis=0) for s in spans]
    trunks = gather_trunks(owns[0], group_count)
    zero = my_group * 0
    place = [my_group]
    for node in range(node_count):
        place += [zero + node, zero]
    attended, query_grads, own_grads, (near, far) = attention(
        parents,
        jnp.stack(place),
        [query_all[s] for s in spans],
        owns,
        output_gradient,
        trunks,
        per_key,
        scaling,
    )
    total = return_parts(near, far, group_count)
    grads = [own_grads[0] + total] + [own_grads[node] for node in range(1, node_count)]
    key_grad = jnp.concatenate([g[:NODE_TOKENS] for g in grads], axis=0).astype(jnp.bfloat16)
    value_grad = jnp.concatenate([g[NODE_TOKENS:] for g in grads], axis=0).astype(jnp.bfloat16)
    query_gradient = jnp.concatenate(query_grads, axis=0)
    query_home, key_home, value_home = [
        lax.all_to_all(a, "head", split_axis=0, concat_axis=1, tiled=True)
        for a in (query_gradient, key_grad, value_grad)
    ]
    return (attended, query_home, key_home, value_home)


def per_device(queries, keys, values, output_gradient, parents):
    node_count = output_gradient.shape[0] // NODE_TOKENS
    per_key = queries.shape[1] // keys.shape[1]
    scaling = 1.0 / math.sqrt(HEAD_SIZE)
    paired = lax.axis_size("head") == 2 and node_count == 2
    body = paired_device if paired else general_device
    return body(queries, keys, values, output_gradient, parents, per_key, scaling)


def solution(mesh):
    placed = (
        P(("leaf", "head"), None),
        P(("leaf", "head"), None),
        P(("leaf", "head"), None),
        P("leaf", "head"),
        P(),
    )
    return jax.shard_map(
        per_device,
        mesh=mesh,
        in_specs=placed,
        out_specs=(
            P("leaf", "head"),
            P(("leaf", "head"), None),
            P(("leaf", "head"), None),
            P(("leaf", "head"), None),
        ),
        check_vma=False,
    )
```

```python
import functools
import math

import jax
import jax.numpy as jnp
from jax import lax
from jax.experimental import pallas as pl
from jax.experimental.pallas import tpu as pltpu
from jax.sharding import PartitionSpec as P


HEAD_SIZE = 128
NODE_TOKENS = 128
MAX_DEPTH = 6

masked_score = -1e30
TILE_HEADS = 2
KERNEL_BYTES = 24 * 2**20


def exchange_bits(count):
    bits = []
    bit = count // 2
    while bit:
        bits.append(bit)
        bit //= 2
    return bits


def reverse_bits(value, count):
    result = value * 0
    bit, mirrored = 1, count // 2
    while mirrored:
        result = result + jnp.where((value & bit) != 0, mirrored, 0)
        bit, mirrored = bit * 2, mirrored // 2
    return result


def ring_size(group_count):
    return 4 if group_count % 4 == 0 else 1


def relative_spots(me, target, group_count):
    ring = ring_size(group_count)
    inner = group_count // ring
    me_ring, target_ring = me // inner, target // inner
    block = ring * reverse_bits((me % inner) ^ (target % inner), inner)
    gathered = block + (me_ring - target_ring + ring) % ring
    returned = block + (target_ring - me_ring + ring) % ring
    return gathered, returned


def attention_kernel(
    group_count,
    node_count,
    per_key,
    scaling,
    parents_ref,
    place_ref,
    *refs,
):
    query_refs = refs[:node_count]
    own_refs = refs[node_count : 2 * node_count]
    grad_refs = refs[2 * node_count : 3 * node_count]
    trunk_ref = refs[3 * node_count]
    outs = refs[3 * node_count + 1 :]
    attended_ref = outs[0]
    query_grad_refs = outs[1 : 1 + node_count]
    own_grad_ref, near_ref, far_ref = outs[1 + node_count : 4 + node_count]
    keys_s, values_s, keys_t, values_t, weight_f, weight_b, score_b, key_acc, value_acc = outs[
        4 + node_count :
    ]
    factor = scaling * math.log2(math.e)
    trunk_rows = MAX_DEPTH * NODE_TOKENS
    half = group_count // 2
    tile_rows = TILE_HEADS * NODE_TOKENS
    me = place_ref[0]
    current = parents_ref[me]
    spots, back_spots, valids = [], [], []
    for _ in range(MAX_DEPTH):
        valids.append(current >= 0)
        guarded = jnp.maximum(current, 0)
        gathered, returned = relative_spots(me, guarded, group_count)
        spots.append(gathered)
        back_spots.append(returned)
        current = jnp.where(current >= 0, parents_ref[guarded], -1)
    penalties = [jnp.where(valid, 0.0, -masked_score).astype(jnp.float32) for valid in valids]
    penalties.append(None)
    contract_minor = (((1,), (1,)), ((), ()))
    plain = (((1,), (0,)), ((), ()))

    def dot(left, right, dims):
        return lax.dot_general(left, right, dims, preferred_element_type=jnp.float32)

    def place_block(block, key, value):
        rows = slice(block * NODE_TOKENS, (block + 1) * NODE_TOKENS)
        keys_s[rows, :] = key
        values_s[rows, :] = value
        keys_t[:, rows] = key.T
        values_t[:, rows] = value.T

    for level in range(MAX_DEPTH):
        pair = trunk_ref[spots[level]]
        place_block(level, pair[:NODE_TOKENS], pair[NODE_TOKENS:])
    for node in range(node_count):
        own = own_refs[node]
        place_block(MAX_DEPTH + node, own[:NODE_TOKENS, :], own[NODE_TOKENS:, :])
    positions_k = lax.broadcasted_iota(jnp.int32, (NODE_TOKENS, tile_rows), 0)
    positions_q = lax.broadcasted_iota(jnp.int32, (NODE_TOKENS, tile_rows), 1) % NODE_TOKENS
    causal = positions_k <= positions_q
    started = set()

    def block_rows(block):
        return slice(block * NODE_TOKENS, (block + 1) * NODE_TOKENS)

    class Tile:
        def __init__(self, index, node, first_head):
            self.slot = index % 2
            self.node = node
            self.first_head = first_head
            self.blocks = list(range(MAX_DEPTH)) + [MAX_DEPTH + node]
            self.node_rows = pl.ds(
                pl.multiple_of(place_ref[1 + node] * NODE_TOKENS, NODE_TOKENS), NODE_TOKENS
            )

        def columns(self, i):
            start = (self.first_head + i) * HEAD_SIZE
            return slice(start, start + HEAD_SIZE)

        def query(self):
            pieces = [query_refs[self.node][:, self.columns(i)] for i in range(TILE_HEADS)]
            return jnp.concatenate(pieces, axis=0)

        def forward(self):
            query = self.query()
            top = None
            for b, block in enumerate(self.blocks):
                scores = dot(keys_s[block_rows(block), :], query, contract_minor)
                if b == MAX_DEPTH:
                    scores = jnp.where(causal, scores, masked_score)
                weight_f[self.slot, block_rows(b), :] = scores
                peak = jnp.max(scores, axis=0, keepdims=True)
                if b < MAX_DEPTH:
                    peak = peak - penalties[b]
                top = peak if top is None else jnp.maximum(top, peak)
                yield
            weight_sum = None
            for b in range(MAX_DEPTH + 1):
                shift = top if b == MAX_DEPTH else top + penalties[b]
                weight = jnp.exp2((weight_f[self.slot, block_rows(b), :] - shift) * factor)
                weight_f[self.slot, block_rows(b), :] = weight
                weight_b[self.slot, block_rows(b), :] = weight.astype(jnp.bfloat16)
                addition = jnp.sum(weight, axis=0, keepdims=True)
                weight_sum = addition if weight_sum is None else weight_sum + addition
                yield
            self.inverse = 1.0 / weight_sum

        def backward(self):
            grad_t = jnp.concatenate(
                [grad_refs[self.node][:, self.columns(i)].T for i in range(TILE_HEADS)],
                axis=1,
            )
            scaled_t = (grad_t.astype(jnp.float32) * self.inverse).astype(jnp.bfloat16)
            trunk = slice(0, trunk_rows)
            own_block = self.blocks[-1]
            attended = dot(values_t[:, trunk], weight_b[self.slot, trunk, :], plain)
            attended += dot(
                values_t[:, block_rows(own_block)],
                weight_b[self.slot, block_rows(MAX_DEPTH), :],
                plain,
            )
            attended = (attended * self.inverse).astype(jnp.bfloat16)
            delta = jnp.sum(
                attended.astype(jnp.float32) * scaled_t.astype(jnp.float32),
                axis=0,
                keepdims=True,
            )
            for i in range(TILE_HEADS):
                attended_ref[self.node_rows, self.columns(i)] = attended[
                    :, block_rows(i)
                ].T
            yield
            for b, block in enumerate(self.blocks):
                prob_grad = dot(values_s[block_rows(block), :], scaled_t, plain)
                weight = weight_f[self.slot, block_rows(b), :]
                score_b[self.slot, block_rows(b), :] = (weight * (prob_grad - delta)).astype(
                    jnp.bfloat16
                )
                yield
            query = self.query()
            for b, block in enumerate(self.blocks):
                key_part = dot(score_b[self.slot, block_rows(b), :], query, plain)
                value_part = dot(weight_b[self.slot, block_rows(b), :], scaled_t, contract_minor)
                if block in started:
                    key_acc[block_rows(block), :] += key_part
                    value_acc[block_rows(block), :] += value_part
                else:
                    key_acc[block_rows(block), :] = key_part
                    value_acc[block_rows(block), :] = value_part
                    started.add(block)
                yield
            query_grad = dot(keys_t[:, trunk], score_b[self.slot, trunk, :], plain)
            query_grad += dot(
                keys_t[:, block_rows(own_block)],
                score_b[self.slot, block_rows(MAX_DEPTH), :],
                plain,
            )
            query_grad = (query_grad * scaling).astype(jnp.bfloat16)
            for i in range(TILE_HEADS):
                query_grad_refs[self.node][:, self.columns(i)] = query_grad[
                    :, block_rows(i)
                ].T
            yield

    tiles = []
    for node in range(node_count):
        for first_head in range(0, per_key, TILE_HEADS):
            tiles.append(Tile(len(tiles), node, first_head))
    before = iter(())
    for tile in tiles + [None]:
        running = [before] + ([tile.forward()] if tile is not None else [])
        while running:
            for stream in list(running):
                if next(stream, running) is running:
                    running.remove(stream)
        before = tile.backward() if tile is not None else iter(())

    for node in range(node_count):
        rows = block_rows(MAX_DEPTH + node)
        own_grad_ref[node, :NODE_TOKENS, :] = key_acc[rows, :] * scaling
        own_grad_ref[node, NODE_TOKENS:, :] = value_acc[rows, :]
    near_ref[...] = jnp.zeros(near_ref.shape, near_ref.dtype)
    far_ref[...] = jnp.zeros(far_ref.shape, far_ref.dtype)
    for level in range(MAX_DEPTH):

        def store(part_ref, spot, rows=block_rows(level)):
            part_ref[spot, :NODE_TOKENS, :] = (key_acc[rows, :] * scaling).astype(part_ref.dtype)
            part_ref[spot, NODE_TOKENS:, :] = value_acc[rows, :].astype(part_ref.dtype)

        spot = back_spots[level]
        pl.when(valids[level] & (spot < half))(functools.partial(store, near_ref, spot))
        pl.when(valids[level] & (spot >= half))(functools.partial(store, far_ref, spot - half))


def on_chip(array):
    return pltpu.with_memory_space_constraint(array, pltpu.VMEM)


def attention(parents, place, queries, owns, grads, trunks, per_key, scaling):
    node_count = len(queries)
    group_count = trunks.shape[0]
    width = per_key * HEAD_SIZE
    block_count = MAX_DEPTH + node_count
    held_rows = block_count * NODE_TOKENS
    seen_rows = (MAX_DEPTH + 1) * NODE_TOKENS
    tile_rows = TILE_HEADS * NODE_TOKENS
    bf16, f32 = jnp.bfloat16, jnp.float32
    smem = pl.BlockSpec(memory_space=pltpu.SMEM)
    vmem = pl.BlockSpec(memory_space=pltpu.VMEM)
    half_shape = pltpu.VMEM((group_count // 2, 2 * NODE_TOKENS, HEAD_SIZE), bf16)
    out_shape = (
        [pltpu.VMEM((node_count * NODE_TOKENS, width), bf16)]
        + [pltpu.VMEM((NODE_TOKENS, width), bf16)] * node_count
        + [pltpu.VMEM((node_count, 2 * NODE_TOKENS, HEAD_SIZE), f32)]
        + [half_shape, half_shape]
    )
    pairs = node_count * per_key * NODE_TOKENS * seen_rows
    results = pl.pallas_call(
        functools.partial(attention_kernel, group_count, node_count, per_key, scaling),
        out_shape=out_shape,
        in_specs=[smem, smem] + [vmem] * (3 * node_count + 1),
        out_specs=[vmem] * len(out_shape),
        scratch_shapes=[
            pltpu.VMEM((held_rows, HEAD_SIZE), bf16),
            pltpu.VMEM((held_rows, HEAD_SIZE), bf16),
            pltpu.VMEM((HEAD_SIZE, held_rows), bf16),
            pltpu.VMEM((HEAD_SIZE, held_rows), bf16),
            pltpu.VMEM((2, seen_rows, tile_rows), f32),
            pltpu.VMEM((2, seen_rows, tile_rows), bf16),
            pltpu.VMEM((2, seen_rows, tile_rows), bf16),
            pltpu.VMEM((held_rows, HEAD_SIZE), f32),
            pltpu.VMEM((held_rows, HEAD_SIZE), f32),
        ],
        compiler_params=pltpu.CompilerParams(vmem_limit_bytes=KERNEL_BYTES),
        cost_estimate=pl.CostEstimate(
            flops=12 * pairs * HEAD_SIZE, transcendentals=pairs, bytes_accessed=8 * 2**20
        ),
    )(
        parents,
        place,
        *[on_chip(a) for a in (*queries, *owns, *grads, trunks)],
    )
    attended = results[0]
    query_grads = results[1 : 1 + node_count]
    own_grads = results[1 + node_count]
    parts = results[2 + node_count :]
    return attended, query_grads, own_grads, parts


def partner_pairs(count, bit):
    return [(i, i ^ bit) for i in range(count)]


def ring_pairs(count, shift):
    ring = ring_size(count)
    inner = count // ring
    return [(i, (i // inner + shift) % ring * inner + i % inner) for i in range(count)]


def gather_trunks(trunk, group_count):
    ring = ring_size(group_count)
    pieces = [trunk]
    for shift in range(1, ring):
        pieces.append(lax.ppermute(trunk, "leaf", ring_pairs(group_count, shift)))
    middle = (ring + 1) // 2
    held = jnp.stack(pieces)
    for stage, bit in enumerate(exchange_bits(group_count // ring)):
        pairs = partner_pairs(group_count, bit)
        sent = [held]
        if stage == 0 and ring > 1:
            sent = [jnp.stack(pieces[:middle]), jnp.stack(pieces[middle:])]
        arrived = []
        for part in sent:
            arrived.append(lax.ppermute(part, "leaf", pairs))
        held = jnp.concatenate([held, *arrived], axis=0)
    return held


def merged(near, arrived):
    return (near.astype(jnp.float32) + arrived.astype(jnp.float32)).astype(jnp.bfloat16)


def return_parts(near, far, group_count):
    ring = ring_size(group_count)
    middle = (ring + 1) // 2
    bits = exchange_bits(group_count // ring)
    for bit in reversed(bits):
        pairs = partner_pairs(group_count, bit)
        if far.shape[0] == ring and ring > 1:
            late = lax.ppermute(far[middle:], "leaf", pairs)
            early = lax.ppermute(far[:middle], "leaf", pairs)
            early, late = merged(near[:middle], early), merged(near[middle:], late)
            blocks = [early[i] for i in range(middle)] + [late[i] for i in range(ring - middle)]
        else:
            arrived = lax.ppermute(far, "leaf", pairs)
            total = merged(near, arrived)
            half = near.shape[0] // 2
            near, far = total[:half], total[half:]
            blocks = [total[0]]
    total = blocks[0].astype(jnp.float32)
    for shift in range(1, ring):
        arrived = lax.ppermute(blocks[shift], "leaf", ring_pairs(group_count, shift))
        total = total + arrived.astype(jnp.float32)
    return total


def pair_of(arrays, columns):
    return jnp.concatenate([array[:, columns] for array in arrays], axis=0)


def paired_device(queries, keys, values, output_gradient, parents, per_key, scaling):
    group_count = lax.axis_size("leaf")
    my_head = lax.axis_index("head")
    my_group = lax.axis_index("leaf").astype(jnp.int32)
    width = output_gradient.shape[1]
    swap = [(0, 1), (1, 0)]
    first = my_head == 0
    other = 1 - my_head
    pair0 = pair_of((keys, values), slice(0, HEAD_SIZE))
    pair1 = pair_of((keys, values), slice(HEAD_SIZE, 2 * HEAD_SIZE))
    kept = jnp.where(first, pair0, pair1)
    came = lax.ppermute(jnp.where(first, pair1, pair0), "head", swap)
    query_send = lax.dynamic_slice_in_dim(queries, other * width, width, 1)
    query_kept = lax.dynamic_slice_in_dim(queries, my_head * width, width, 1)
    grads = [
        lax.dynamic_slice_in_dim(output_gradient, node * NODE_TOKENS, NODE_TOKENS, 0)
        for node in (my_head, other)
    ]
    query_came = lax.ppermute(query_send, "head", swap)
    trunks = gather_trunks(jnp.where(first, kept, came), group_count)
    place = jnp.stack([my_group, my_head, other]).astype(jnp.int32)
    attended, query_grads, own_grads, (near, far) = attention(
        parents,
        place,
        [query_kept, query_came],
        [kept, came],
        grads,
        trunks,
        per_key,
        scaling,
    )
    query_back = lax.ppermute(query_grads[1], "head", swap)
    total = return_parts(near, far, group_count)
    nothing = jnp.zeros_like(total)
    mine = (own_grads[0] + jnp.where(first, total, nothing)).astype(jnp.bfloat16)
    theirs = (own_grads[1] + jnp.where(first, nothing, total)).astype(jnp.bfloat16)
    came_back = lax.ppermute(theirs, "head", swap)
    left = jnp.where(first, mine, came_back)
    right = jnp.where(first, came_back, mine)
    key_home = jnp.concatenate([left[:NODE_TOKENS], right[:NODE_TOKENS]], axis=1)
    value_home = jnp.concatenate([left[NODE_TOKENS:], right[NODE_TOKENS:]], axis=1)
    query_home = jnp.concatenate(
        [
            jnp.where(first, query_grads[0], query_back),
            jnp.where(first, query_back, query_grads[0]),
        ],
        axis=1,
    )
    return (attended, query_home, key_home, value_home)


def general_device(queries, keys, values, output_gradient, parents, per_key, scaling):
    group_count = lax.axis_size("leaf")
    my_group = lax.axis_index("leaf").astype(jnp.int32)
    node_count = output_gradient.shape[0] // NODE_TOKENS
    query_all, key_all, value_all = [
        lax.all_to_all(a, "head", split_axis=1, concat_axis=0, tiled=True)
        for a in (queries, keys, values)
    ]
    spans = [slice(n * NODE_TOKENS, (n + 1) * NODE_TOKENS) for n in range(node_count)]
    owns = [jnp.concatenate([key_all[s], value_all[s]], axis=0) for s in spans]
    trunks = gather_trunks(owns[0], group_count)
    zero = my_group * 0
    place = [my_group]
    for node in range(node_count):
        place += [zero + node]
    attended, query_grads, own_grads, (near, far) = attention(
        parents,
        jnp.stack(place),
        [query_all[s] for s in spans],
        owns,
        [output_gradient[s] for s in spans],
        trunks,
        per_key,
        scaling,
    )
    total = return_parts(near, far, group_count)
    grads = [own_grads[0] + total] + [own_grads[node] for node in range(1, node_count)]
    key_grad = jnp.concatenate([g[:NODE_TOKENS] for g in grads], axis=0).astype(jnp.bfloat16)
    value_grad = jnp.concatenate([g[NODE_TOKENS:] for g in grads], axis=0).astype(jnp.bfloat16)
    query_gradient = jnp.concatenate(query_grads, axis=0)
    query_home, key_home, value_home = [
        lax.all_to_all(a, "head", split_axis=0, concat_axis=1, tiled=True)
        for a in (query_gradient, key_grad, value_grad)
    ]
    return (attended, query_home, key_home, value_home)


def per_device(queries, keys, values, output_gradient, parents):
    node_count = output_gradient.shape[0] // NODE_TOKENS
    per_key = queries.shape[1] // keys.shape[1]
    scaling = 1.0 / math.sqrt(HEAD_SIZE)
    paired = lax.axis_size("head") == 2 and node_count == 2
    body = paired_device if paired else general_device
    return body(queries, keys, values, output_gradient, parents, per_key, scaling)


def solution(mesh):
    placed = (
        P(("leaf", "head"), None),
        P(("leaf", "head"), None),
        P(("leaf", "head"), None),
        P("leaf", "head"),
        P(),
    )
    return jax.shard_map(
        per_device,
        mesh=mesh,
        in_specs=placed,
        out_specs=(
            P("leaf", "head"),
            P(("leaf", "head"), None),
            P(("leaf", "head"), None),
            P(("leaf", "head"), None),
        ),
        check_vma=False,
    )
```

```python
import functools
import math

import jax
import jax.numpy as jnp
from jax import lax
from jax.experimental import pallas as pl
from jax.experimental.pallas import tpu as pltpu
from jax.sharding import PartitionSpec as P


HEAD_SIZE = 128
NODE_TOKENS = 128
MAX_DEPTH = 6

masked_score = -1e30
TILE_HEADS = 2
KERNEL_BYTES = 24 * 2**20


def exchange_bits(count):
    bits = []
    bit = count // 2
    while bit:
        bits.append(bit)
        bit //= 2
    return bits


def reverse_bits(value, count):
    result = value * 0
    bit, mirrored = 1, count // 2
    while mirrored:
        result = result + jnp.where((value & bit) != 0, mirrored, 0)
        bit, mirrored = bit * 2, mirrored // 2
    return result


def ring_size(group_count):
    return 4 if group_count % 4 == 0 else 1


def relative_spots(me, target, group_count):
    ring = ring_size(group_count)
    inner = group_count // ring
    me_ring, target_ring = me // inner, target // inner
    block = ring * reverse_bits((me % inner) ^ (target % inner), inner)
    gathered = block + (me_ring - target_ring + ring) % ring
    returned = block + (target_ring - me_ring + ring) % ring
    return gathered, returned


def attention_kernel(
    group_count,
    node_count,
    per_key,
    scaling,
    parents_ref,
    place_ref,
    *refs,
):
    query_refs = refs[:node_count]
    own_refs = refs[node_count : 2 * node_count]
    grad_refs = refs[2 * node_count : 3 * node_count]
    trunk_ref = refs[3 * node_count]
    outs = refs[3 * node_count + 1 :]
    attended_ref, near_ref, far_ref, keys_s = outs[:4]
    score_refs, weight_refs, scaled_refs = [
        outs[4 + i * node_count : 4 + (i + 1) * node_count] for i in range(3)
    ]
    values_s, values_t, weight_f, weight_b, key_acc, value_acc = outs[4 + 3 * node_count :]
    factor = scaling * math.log2(math.e)
    trunk_rows = MAX_DEPTH * NODE_TOKENS
    half = group_count // 2
    tile_rows = TILE_HEADS * NODE_TOKENS
    me = place_ref[0]
    current = parents_ref[me]
    spots, back_spots, valids = [], [], []
    for _ in range(MAX_DEPTH):
        valids.append(current >= 0)
        guarded = jnp.maximum(current, 0)
        gathered, returned = relative_spots(me, guarded, group_count)
        spots.append(gathered)
        back_spots.append(returned)
        current = jnp.where(current >= 0, parents_ref[guarded], -1)
    penalties = [jnp.where(valid, 0.0, -masked_score).astype(jnp.float32) for valid in valids]
    penalties.append(None)
    contract_minor = (((1,), (1,)), ((), ()))
    plain = (((1,), (0,)), ((), ()))

    def dot(left, right, dims):
        return lax.dot_general(left, right, dims, preferred_element_type=jnp.float32)

    def place_block(block, key, value):
        rows = slice(block * NODE_TOKENS, (block + 1) * NODE_TOKENS)
        keys_s[rows, :] = key
        values_s[rows, :] = value
        values_t[:, rows] = value.T

    for level in range(MAX_DEPTH):
        pair = trunk_ref[spots[level]]
        place_block(level, pair[:NODE_TOKENS], pair[NODE_TOKENS:])
    for node in range(node_count):
        own = own_refs[node]
        place_block(MAX_DEPTH + node, own[:NODE_TOKENS, :], own[NODE_TOKENS:, :])
    positions_k = lax.broadcasted_iota(jnp.int32, (NODE_TOKENS, tile_rows), 0)
    positions_q = lax.broadcasted_iota(jnp.int32, (NODE_TOKENS, tile_rows), 1) % NODE_TOKENS
    causal = positions_k <= positions_q
    started = set()

    def block_rows(block):
        return slice(block * NODE_TOKENS, (block + 1) * NODE_TOKENS)

    class Tile:
        def __init__(self, index, node, first_head):
            self.slot = index % 2
            self.node = node
            self.first_head = first_head
            self.number = first_head // TILE_HEADS
            self.blocks = list(range(MAX_DEPTH)) + [MAX_DEPTH + node]
            self.node_rows = pl.ds(
                pl.multiple_of(place_ref[1 + node] * NODE_TOKENS, NODE_TOKENS), NODE_TOKENS
            )

        def columns(self, i):
            start = (self.first_head + i) * HEAD_SIZE
            return slice(start, start + HEAD_SIZE)

        def query(self):
            pieces = [query_refs[self.node][:, self.columns(i)] for i in range(TILE_HEADS)]
            return jnp.concatenate(pieces, axis=0)

        def forward(self):
            query = self.query()
            top = None
            for b, block in enumerate(self.blocks):
                scores = dot(keys_s[block_rows(block), :], query, contract_minor)
                if b == MAX_DEPTH:
                    scores = jnp.where(causal, scores, masked_score)
                weight_f[self.slot, block_rows(b), :] = scores
                peak = jnp.max(scores, axis=0, keepdims=True)
                if b < MAX_DEPTH:
                    peak = peak - penalties[b]
                top = peak if top is None else jnp.maximum(top, peak)
                yield
            weight_sum = None
            for b in range(MAX_DEPTH + 1):
                shift = top if b == MAX_DEPTH else top + penalties[b]
                weight = jnp.exp2((weight_f[self.slot, block_rows(b), :] - shift) * factor)
                weight_f[self.slot, block_rows(b), :] = weight
                weight_b[self.slot, block_rows(b), :] = weight.astype(jnp.bfloat16)
                addition = jnp.sum(weight, axis=0, keepdims=True)
                weight_sum = addition if weight_sum is None else weight_sum + addition
                yield
            self.inverse = 1.0 / weight_sum

        def backward(self):
            grad_t = jnp.concatenate(
                [grad_refs[self.node][:, self.columns(i)].T for i in range(TILE_HEADS)],
                axis=1,
            )
            scaled_t = (grad_t.astype(jnp.float32) * self.inverse).astype(jnp.bfloat16)
            score_b = score_refs[self.node]
            scaled_refs[self.node][self.number] = scaled_t
            weight_refs[self.node][self.number] = weight_b[self.slot, block_rows(MAX_DEPTH), :]
            trunk = slice(0, trunk_rows)
            own_block = self.blocks[-1]
            attended = dot(values_t[:, trunk], weight_b[self.slot, trunk, :], plain)
            attended += dot(
                values_t[:, block_rows(own_block)],
                weight_b[self.slot, block_rows(MAX_DEPTH), :],
                plain,
            )
            attended = (attended * self.inverse).astype(jnp.bfloat16)
            delta = jnp.sum(
                attended.astype(jnp.float32) * scaled_t.astype(jnp.float32),
                axis=0,
                keepdims=True,
            )
            for i in range(TILE_HEADS):
                attended_ref[self.node_rows, self.columns(i)] = attended[
                    :, block_rows(i)
                ].T
            yield
            for b, block in enumerate(self.blocks):
                prob_grad = dot(values_s[block_rows(block), :], scaled_t, plain)
                weight = weight_f[self.slot, block_rows(b), :]
                score_b[self.number, block_rows(b), :] = (weight * (prob_grad - delta)).astype(
                    jnp.bfloat16
                )
                yield
            query = self.query()
            for b, block in enumerate(self.blocks[:-1]):
                key_part = dot(score_b[self.number, block_rows(b), :], query, plain)
                value_part = dot(weight_b[self.slot, block_rows(b), :], scaled_t, contract_minor)
                if block in started:
                    key_acc[block_rows(block), :] += key_part
                    value_acc[block_rows(block), :] += value_part
                else:
                    key_acc[block_rows(block), :] = key_part
                    value_acc[block_rows(block), :] = value_part
                    started.add(block)
                yield

    tiles = []
    for node in range(node_count):
        for first_head in range(0, per_key, TILE_HEADS):
            tiles.append(Tile(len(tiles), node, first_head))
    before = iter(())
    for tile in tiles + [None]:
        running = [before] + ([tile.forward()] if tile is not None else [])
        while running:
            for stream in list(running):
                if next(stream, running) is running:
                    running.remove(stream)
        before = tile.backward() if tile is not None else iter(())

    near_ref[...] = jnp.zeros(near_ref.shape, near_ref.dtype)
    far_ref[...] = jnp.zeros(far_ref.shape, far_ref.dtype)
    for level in range(MAX_DEPTH):

        def store(part_ref, spot, rows=block_rows(level)):
            part_ref[spot, :NODE_TOKENS, :] = (key_acc[rows, :] * scaling).astype(part_ref.dtype)
            part_ref[spot, NODE_TOKENS:, :] = value_acc[rows, :].astype(part_ref.dtype)

        spot = back_spots[level]
        pl.when(valids[level] & (spot < half))(functools.partial(store, near_ref, spot))
        pl.when(valids[level] & (spot >= half))(functools.partial(store, far_ref, spot - half))


def finish_kernel(
    node,
    per_key,
    scaling,
    query_ref,
    keys_ref,
    score_ref,
    weight_ref,
    scaled_ref,
    query_grad_ref,
    own_grad_ref,
    keys_t,
):
    contract_minor = (((1,), (1,)), ((), ()))
    plain = (((1,), (0,)), ((), ()))

    def dot(left, right, dims):
        return lax.dot_general(left, right, dims, preferred_element_type=jnp.float32)

    def block_rows(block):
        return slice(block * NODE_TOKENS, (block + 1) * NODE_TOKENS)

    for b, block in enumerate([*range(MAX_DEPTH), MAX_DEPTH + node]):
        keys_t[:, block_rows(b)] = keys_ref[block_rows(block), :].T
    key_total = value_total = None
    for number in range(per_key // TILE_HEADS):
        columns = [
            slice((number * TILE_HEADS + i) * HEAD_SIZE, (number * TILE_HEADS + i + 1) * HEAD_SIZE)
            for i in range(TILE_HEADS)
        ]
        query = jnp.concatenate([query_ref[:, c] for c in columns], axis=0)
        key_part = dot(score_ref[number, block_rows(MAX_DEPTH), :], query, plain)
        value_part = dot(weight_ref[number], scaled_ref[number], contract_minor)
        key_total = key_part if key_total is None else key_total + key_part
        value_total = value_part if value_total is None else value_total + value_part
        query_grad = (dot(keys_t[...], score_ref[number], plain) * scaling).astype(jnp.bfloat16)
        for i, c in enumerate(columns):
            query_grad_ref[:, c] = query_grad[:, block_rows(i)].T
    own_grad_ref[:NODE_TOKENS, :] = key_total * scaling
    own_grad_ref[NODE_TOKENS:, :] = value_total


def finish(node, query, held, per_key, scaling):
    keys_s, scores, weights, scaled = held
    width = per_key * HEAD_SIZE
    seen_rows = (MAX_DEPTH + 1) * NODE_TOKENS
    vmem = pl.BlockSpec(memory_space=pltpu.VMEM)
    operands = (query, keys_s, scores[node], weights[node], scaled[node])
    pairs = per_key * NODE_TOKENS * seen_rows
    return pl.pallas_call(
        functools.partial(finish_kernel, node, per_key, scaling),
        out_shape=[
            pltpu.VMEM((NODE_TOKENS, width), jnp.bfloat16),
            pltpu.VMEM((2 * NODE_TOKENS, HEAD_SIZE), jnp.float32),
        ],
        in_specs=[vmem] * len(operands),
        out_specs=[vmem] * 2,
        scratch_shapes=[pltpu.VMEM((HEAD_SIZE, seen_rows), jnp.bfloat16)],
        compiler_params=pltpu.CompilerParams(vmem_limit_bytes=KERNEL_BYTES // 2),
        cost_estimate=pl.CostEstimate(
            flops=2 * pairs * HEAD_SIZE, transcendentals=0, bytes_accessed=2**20
        ),
    )(*[on_chip(a) for a in operands])


def on_chip(array):
    return pltpu.with_memory_space_constraint(array, pltpu.VMEM)


def attention(parents, place, queries, owns, grads, trunks, per_key, scaling):
    node_count = len(queries)
    group_count = trunks.shape[0]
    width = per_key * HEAD_SIZE
    tile_count = per_key // TILE_HEADS
    held_rows = (MAX_DEPTH + node_count) * NODE_TOKENS
    seen_rows = (MAX_DEPTH + 1) * NODE_TOKENS
    tile_rows = TILE_HEADS * NODE_TOKENS
    bf16, f32 = jnp.bfloat16, jnp.float32
    smem = pl.BlockSpec(memory_space=pltpu.SMEM)
    vmem = pl.BlockSpec(memory_space=pltpu.VMEM)
    half_shape = pltpu.VMEM((group_count // 2, 2 * NODE_TOKENS, HEAD_SIZE), bf16)
    out_shape = (
        [pltpu.VMEM((node_count * NODE_TOKENS, width), bf16), half_shape, half_shape]
        + [pltpu.VMEM((held_rows, HEAD_SIZE), bf16)]
        + [pltpu.VMEM((tile_count, seen_rows, tile_rows), bf16)] * node_count
        + [pltpu.VMEM((tile_count, NODE_TOKENS, tile_rows), bf16)] * node_count
        + [pltpu.VMEM((tile_count, HEAD_SIZE, tile_rows), bf16)] * node_count
    )
    pairs = node_count * per_key * NODE_TOKENS * seen_rows
    results = pl.pallas_call(
        functools.partial(attention_kernel, group_count, node_count, per_key, scaling),
        out_shape=out_shape,
        in_specs=[smem, smem] + [vmem] * (3 * node_count + 1),
        out_specs=[vmem] * len(out_shape),
        scratch_shapes=[
            pltpu.VMEM((held_rows, HEAD_SIZE), bf16),
            pltpu.VMEM((HEAD_SIZE, held_rows), bf16),
            pltpu.VMEM((2, seen_rows, tile_rows), f32),
            pltpu.VMEM((2, seen_rows, tile_rows), bf16),
            pltpu.VMEM((MAX_DEPTH * NODE_TOKENS, HEAD_SIZE), f32),
            pltpu.VMEM((MAX_DEPTH * NODE_TOKENS, HEAD_SIZE), f32),
        ],
        compiler_params=pltpu.CompilerParams(vmem_limit_bytes=KERNEL_BYTES),
        cost_estimate=pl.CostEstimate(
            flops=10 * pairs * HEAD_SIZE, transcendentals=pairs, bytes_accessed=8 * 2**20
        ),
    )(
        parents,
        place,
        *[on_chip(a) for a in (*queries, *owns, *grads, trunks)],
    )
    attended, near, far, keys_s = results[:4]
    scores, weights, scaled = [
        results[4 + i * node_count : 4 + (i + 1) * node_count] for i in range(3)
    ]
    return attended, (near, far), (keys_s, scores, weights, scaled)


def partner_pairs(count, bit):
    return [(i, i ^ bit) for i in range(count)]


def ring_pairs(count, shift):
    ring = ring_size(count)
    inner = count // ring
    return [(i, (i // inner + shift) % ring * inner + i % inner) for i in range(count)]


def gather_trunks(trunk, group_count):
    ring = ring_size(group_count)
    pieces = [trunk]
    for shift in range(1, ring):
        pieces.append(lax.ppermute(trunk, "leaf", ring_pairs(group_count, shift)))
    middle = (ring + 1) // 2
    held = jnp.stack(pieces)
    for stage, bit in enumerate(exchange_bits(group_count // ring)):
        pairs = partner_pairs(group_count, bit)
        sent = [held]
        if stage == 0 and ring > 1:
            sent = [jnp.stack(pieces[:middle]), jnp.stack(pieces[middle:])]
        arrived = []
        for part in sent:
            arrived.append(lax.ppermute(part, "leaf", pairs))
        held = jnp.concatenate([held, *arrived], axis=0)
    return held


def merged(near, arrived):
    return (near.astype(jnp.float32) + arrived.astype(jnp.float32)).astype(jnp.bfloat16)


def return_parts(near, far, group_count):
    ring = ring_size(group_count)
    middle = (ring + 1) // 2
    bits = exchange_bits(group_count // ring)
    for bit in reversed(bits):
        pairs = partner_pairs(group_count, bit)
        if far.shape[0] == ring and ring > 1:
            late = lax.ppermute(far[middle:], "leaf", pairs)
            early = lax.ppermute(far[:middle], "leaf", pairs)
            late = merged(near[middle:], late)
            early, _ = lax.optimization_barrier((early, late))
            early = merged(near[:middle], early)
            blocks = [early[i] for i in range(middle)] + [late[i] for i in range(ring - middle)]
        else:
            arrived = lax.ppermute(far, "leaf", pairs)
            total = merged(near, arrived)
            half = near.shape[0] // 2
            near, far = total[:half], total[half:]
            blocks = [total[0]]
    total = blocks[0].astype(jnp.float32)
    for shift in range(1, ring):
        arrived = lax.ppermute(blocks[shift], "leaf", ring_pairs(group_count, shift))
        total = total + arrived.astype(jnp.float32)
    return total


def pair_of(arrays, columns):
    return jnp.concatenate([array[:, columns] for array in arrays], axis=0)


def paired_device(queries, keys, values, output_gradient, parents, per_key, scaling):
    group_count = lax.axis_size("leaf")
    my_head = lax.axis_index("head")
    my_group = lax.axis_index("leaf").astype(jnp.int32)
    width = output_gradient.shape[1]
    swap = [(0, 1), (1, 0)]
    first = my_head == 0
    other = 1 - my_head
    pair0 = pair_of((keys, values), slice(0, HEAD_SIZE))
    pair1 = pair_of((keys, values), slice(HEAD_SIZE, 2 * HEAD_SIZE))
    kept = jnp.where(first, pair0, pair1)
    came = lax.ppermute(jnp.where(first, pair1, pair0), "head", swap)
    query_send = lax.dynamic_slice_in_dim(queries, other * width, width, 1)
    query_kept = lax.dynamic_slice_in_dim(queries, my_head * width, width, 1)
    grads = [
        lax.dynamic_slice_in_dim(output_gradient, node * NODE_TOKENS, NODE_TOKENS, 0)
        for node in (my_head, other)
    ]
    query_came = lax.ppermute(query_send, "head", swap)
    trunks = gather_trunks(jnp.where(first, kept, came), group_count)
    place = jnp.stack([my_group, my_head, other]).astype(jnp.int32)
    query_nodes = [query_kept, query_came]
    attended, (near, far), held = attention(
        parents,
        place,
        query_nodes,
        [kept, came],
        grads,
        trunks,
        per_key,
        scaling,
    )
    query_away, own_away = finish(1, query_nodes[1], held, per_key, scaling)
    query_here, own_here = finish(0, query_nodes[0], held, per_key, scaling)
    query_back = lax.ppermute(query_away, "head", swap)
    total = return_parts(near, far, group_count)
    nothing = jnp.zeros_like(total)
    mine = (own_here + jnp.where(first, total, nothing)).astype(jnp.bfloat16)
    theirs = (own_away + jnp.where(first, nothing, total)).astype(jnp.bfloat16)
    came_back = lax.ppermute(theirs, "head", swap)
    left = jnp.where(first, mine, came_back)
    right = jnp.where(first, came_back, mine)
    key_home = jnp.concatenate([left[:NODE_TOKENS], right[:NODE_TOKENS]], axis=1)
    value_home = jnp.concatenate([left[NODE_TOKENS:], right[NODE_TOKENS:]], axis=1)
    query_home = jnp.concatenate(
        [
            jnp.where(first, query_here, query_back),
            jnp.where(first, query_back, query_here),
        ],
        axis=1,
    )
    return (attended, query_home, key_home, value_home)


def general_device(queries, keys, values, output_gradient, parents, per_key, scaling):
    group_count = lax.axis_size("leaf")
    my_group = lax.axis_index("leaf").astype(jnp.int32)
    node_count = output_gradient.shape[0] // NODE_TOKENS
    query_all, key_all, value_all = [
        lax.all_to_all(a, "head", split_axis=1, concat_axis=0, tiled=True)
        for a in (queries, keys, values)
    ]
    spans = [slice(n * NODE_TOKENS, (n + 1) * NODE_TOKENS) for n in range(node_count)]
    owns = [jnp.concatenate([key_all[s], value_all[s]], axis=0) for s in spans]
    trunks = gather_trunks(owns[0], group_count)
    zero = my_group * 0
    place = [my_group]
    for node in range(node_count):
        place += [zero + node]
    query_nodes = [query_all[s] for s in spans]
    attended, (near, far), held = attention(
        parents,
        jnp.stack(place),
        query_nodes,
        owns,
        [output_gradient[s] for s in spans],
        trunks,
        per_key,
        scaling,
    )
    finished = [
        finish(node, query, held, per_key, scaling) for node, query in enumerate(query_nodes)
    ]
    query_grads = [query_grad for query_grad, _ in finished]
    own_grads = [own_grad for _, own_grad in finished]
    total = return_parts(near, far, group_count)
    grads = [own_grads[0] + total] + [own_grads[node] for node in range(1, node_count)]
    key_grad = jnp.concatenate([g[:NODE_TOKENS] for g in grads], axis=0).astype(jnp.bfloat16)
    value_grad = jnp.concatenate([g[NODE_TOKENS:] for g in grads], axis=0).astype(jnp.bfloat16)
    query_gradient = jnp.concatenate(query_grads, axis=0)
    query_home, key_home, value_home = [
        lax.all_to_all(a, "head", split_axis=0, concat_axis=1, tiled=True)
        for a in (query_gradient, key_grad, value_grad)
    ]
    return (attended, query_home, key_home, value_home)


def per_device(queries, keys, values, output_gradient, parents):
    node_count = output_gradient.shape[0] // NODE_TOKENS
    per_key = queries.shape[1] // keys.shape[1]
    scaling = 1.0 / math.sqrt(HEAD_SIZE)
    paired = lax.axis_size("head") == 2 and node_count == 2
    body = paired_device if paired else general_device
    return body(queries, keys, values, output_gradient, parents, per_key, scaling)


def solution(mesh):
    placed = (
        P(("leaf", "head"), None),
        P(("leaf", "head"), None),
        P(("leaf", "head"), None),
        P("leaf", "head"),
        P(),
    )
    return jax.shard_map(
        per_device,
        mesh=mesh,
        in_specs=placed,
        out_specs=(
            P("leaf", "head"),
            P(("leaf", "head"), None),
            P(("leaf", "head"), None),
            P(("leaf", "head"), None),
        ),
        check_vma=False,
    )
```

```python
import functools
import math

import jax
import jax.numpy as jnp
from jax import lax
from jax.experimental import pallas as pl
from jax.experimental.pallas import tpu as pltpu
from jax.sharding import PartitionSpec as P


HEAD_SIZE = 128
NODE_TOKENS = 128
MAX_DEPTH = 6

masked_score = -1e30
TILE_HEADS = 4
KERNEL_BYTES = 24 * 2**20


def exchange_bits(count):
    bits = []
    bit = count // 2
    while bit:
        bits.append(bit)
        bit //= 2
    return bits


def reverse_bits(value, count):
    result = value * 0
    bit, mirrored = 1, count // 2
    while mirrored:
        result = result + jnp.where((value & bit) != 0, mirrored, 0)
        bit, mirrored = bit * 2, mirrored // 2
    return result


def ring_size(group_count):
    return 4 if group_count % 4 == 0 else 1


def ring_order(shift):
    return shift % 2 * 2 + shift // 2


def relative_spots(me, target, group_count):
    ring = ring_size(group_count)
    inner = group_count // ring
    me_ring, target_ring = me // inner, target // inner
    block = ring * reverse_bits((me % inner) ^ (target % inner), inner)
    gathered = block + (me_ring - target_ring + ring) % ring
    returned = block + ring_order((target_ring - me_ring + ring) % ring)
    return gathered, returned


def attention_kernel(
    group_count,
    node_count,
    per_key,
    scaling,
    parents_ref,
    place_ref,
    *refs,
):
    query_refs = refs[:node_count]
    own_refs = refs[node_count : 2 * node_count]
    grad_refs = refs[2 * node_count : 3 * node_count]
    trunk_ref = refs[3 * node_count]
    outs = refs[3 * node_count + 1 :]
    attended_ref, near_ref, far_ref, keys_s = outs[:4]
    score_refs, weight_refs, scaled_refs = [
        outs[4 + i * node_count : 4 + (i + 1) * node_count] for i in range(3)
    ]
    values_s, values_t, weight_f, weight_b, key_acc, value_acc = outs[4 + 3 * node_count :]
    factor = scaling * math.log2(math.e)
    trunk_rows = MAX_DEPTH * NODE_TOKENS
    half = group_count // 2
    tile_rows = TILE_HEADS * NODE_TOKENS
    me = place_ref[0]
    current = parents_ref[me]
    spots, back_spots, valids = [], [], []
    for _ in range(MAX_DEPTH):
        valids.append(current >= 0)
        guarded = jnp.maximum(current, 0)
        gathered, returned = relative_spots(me, guarded, group_count)
        spots.append(gathered)
        back_spots.append(returned)
        current = jnp.where(current >= 0, parents_ref[guarded], -1)
    penalties = [jnp.where(valid, 0.0, -masked_score).astype(jnp.float32) for valid in valids]
    penalties.append(None)
    contract_minor = (((1,), (1,)), ((), ()))
    plain = (((1,), (0,)), ((), ()))

    def dot(left, right, dims):
        return lax.dot_general(left, right, dims, preferred_element_type=jnp.float32)

    def place_block(block, key, value):
        rows = slice(block * NODE_TOKENS, (block + 1) * NODE_TOKENS)
        keys_s[rows, :] = key
        values_s[rows, :] = value
        values_t[:, rows] = value.T

    for level in range(MAX_DEPTH):
        pair = trunk_ref[spots[level]]
        place_block(level, pair[:NODE_TOKENS], pair[NODE_TOKENS:])
    for node in range(node_count):
        own = own_refs[node]
        place_block(MAX_DEPTH + node, own[:NODE_TOKENS, :], own[NODE_TOKENS:, :])
    positions_k = lax.broadcasted_iota(jnp.int32, (NODE_TOKENS, tile_rows), 0)
    positions_q = lax.broadcasted_iota(jnp.int32, (NODE_TOKENS, tile_rows), 1) % NODE_TOKENS
    causal = positions_k <= positions_q
    started = set()

    def block_rows(block):
        return slice(block * NODE_TOKENS, (block + 1) * NODE_TOKENS)

    class Tile:
        def __init__(self, index, node, first_head):
            self.slot = index % 2
            self.node = node
            self.first_head = first_head
            self.number = first_head // TILE_HEADS
            self.blocks = list(range(MAX_DEPTH)) + [MAX_DEPTH + node]
            self.node_rows = pl.ds(
                pl.multiple_of(place_ref[1 + node] * NODE_TOKENS, NODE_TOKENS), NODE_TOKENS
            )

        def columns(self, i):
            start = (self.first_head + i) * HEAD_SIZE
            return slice(start, start + HEAD_SIZE)

        def query(self):
            pieces = [query_refs[self.node][:, self.columns(i)] for i in range(TILE_HEADS)]
            return jnp.concatenate(pieces, axis=0)

        def forward(self):
            query = self.query()
            top = None
            for b, block in enumerate(self.blocks):
                scores = dot(keys_s[block_rows(block), :], query, contract_minor)
                if b == MAX_DEPTH:
                    scores = jnp.where(causal, scores, masked_score)
                weight_f[self.slot, block_rows(b), :] = scores
                peak = jnp.max(scores, axis=0, keepdims=True)
                if b < MAX_DEPTH:
                    peak = peak - penalties[b]
                top = peak if top is None else jnp.maximum(top, peak)
                yield
            weight_sum = None
            for b in range(MAX_DEPTH + 1):
                shift = top if b == MAX_DEPTH else top + penalties[b]
                weight = jnp.exp2((weight_f[self.slot, block_rows(b), :] - shift) * factor)
                weight_f[self.slot, block_rows(b), :] = weight
                weight_b[self.slot, block_rows(b), :] = weight.astype(jnp.bfloat16)
                addition = jnp.sum(weight, axis=0, keepdims=True)
                weight_sum = addition if weight_sum is None else weight_sum + addition
                yield
            self.inverse = 1.0 / weight_sum

        def backward(self):
            grad_t = jnp.concatenate(
                [grad_refs[self.node][:, self.columns(i)].T for i in range(TILE_HEADS)],
                axis=1,
            )
            scaled_t = (grad_t.astype(jnp.float32) * self.inverse).astype(jnp.bfloat16)
            score_b = score_refs[self.node]
            scaled_refs[self.node][self.number] = scaled_t
            weight_refs[self.node][self.number] = weight_b[self.slot, block_rows(MAX_DEPTH), :]
            trunk = slice(0, trunk_rows)
            own_block = self.blocks[-1]
            attended = dot(values_t[:, trunk], weight_b[self.slot, trunk, :], plain)
            attended += dot(
                values_t[:, block_rows(own_block)],
                weight_b[self.slot, block_rows(MAX_DEPTH), :],
                plain,
            )
            attended = (attended * self.inverse).astype(jnp.bfloat16)
            delta = jnp.sum(
                attended.astype(jnp.float32) * scaled_t.astype(jnp.float32),
                axis=0,
                keepdims=True,
            )
            for i in range(TILE_HEADS):
                attended_ref[self.node_rows, self.columns(i)] = attended[
                    :, block_rows(i)
                ].T
            yield
            for b, block in enumerate(self.blocks):
                prob_grad = dot(values_s[block_rows(block), :], scaled_t, plain)
                weight = weight_f[self.slot, block_rows(b), :]
                score_b[self.number, block_rows(b), :] = (weight * (prob_grad - delta)).astype(
                    jnp.bfloat16
                )
                yield
            query = self.query()
            for b, block in enumerate(self.blocks[:-1]):
                key_part = dot(score_b[self.number, block_rows(b), :], query, plain)
                value_part = dot(weight_b[self.slot, block_rows(b), :], scaled_t, contract_minor)
                if block in started:
                    key_acc[block_rows(block), :] += key_part
                    value_acc[block_rows(block), :] += value_part
                else:
                    key_acc[block_rows(block), :] = key_part
                    value_acc[block_rows(block), :] = value_part
                    started.add(block)
                yield

    tiles = []
    for node in range(node_count):
        for first_head in range(0, per_key, TILE_HEADS):
            tiles.append(Tile(len(tiles), node, first_head))
    before = iter(())
    for tile in tiles + [None]:
        running = [before] + ([tile.forward()] if tile is not None else [])
        while running:
            for stream in list(running):
                if next(stream, running) is running:
                    running.remove(stream)
        before = tile.backward() if tile is not None else iter(())

    near_ref[...] = jnp.zeros(near_ref.shape, near_ref.dtype)
    far_ref[...] = jnp.zeros(far_ref.shape, far_ref.dtype)
    for level in range(MAX_DEPTH):

        def store(part_ref, spot, rows=block_rows(level)):
            part_ref[spot, :NODE_TOKENS, :] = (key_acc[rows, :] * scaling).astype(part_ref.dtype)
            part_ref[spot, NODE_TOKENS:, :] = value_acc[rows, :].astype(part_ref.dtype)

        spot = back_spots[level]
        pl.when(valids[level] & (spot < half))(functools.partial(store, near_ref, spot))
        pl.when(valids[level] & (spot >= half))(functools.partial(store, far_ref, spot - half))


def finish_kernel(
    node,
    per_key,
    scaling,
    query_ref,
    keys_ref,
    score_ref,
    weight_ref,
    scaled_ref,
    query_grad_ref,
    own_grad_ref,
    keys_t,
):
    contract_minor = (((1,), (1,)), ((), ()))
    plain = (((1,), (0,)), ((), ()))

    def dot(left, right, dims):
        return lax.dot_general(left, right, dims, preferred_element_type=jnp.float32)

    def block_rows(block):
        return slice(block * NODE_TOKENS, (block + 1) * NODE_TOKENS)

    for b, block in enumerate([*range(MAX_DEPTH), MAX_DEPTH + node]):
        keys_t[:, block_rows(b)] = keys_ref[block_rows(block), :].T
    key_total = value_total = None
    for number in range(per_key // TILE_HEADS):
        columns = [
            slice((number * TILE_HEADS + i) * HEAD_SIZE, (number * TILE_HEADS + i + 1) * HEAD_SIZE)
            for i in range(TILE_HEADS)
        ]
        query = jnp.concatenate([query_ref[:, c] for c in columns], axis=0)
        key_part = dot(score_ref[number, block_rows(MAX_DEPTH), :], query, plain)
        value_part = dot(weight_ref[number], scaled_ref[number], contract_minor)
        key_total = key_part if key_total is None else key_total + key_part
        value_total = value_part if value_total is None else value_total + value_part
        query_grad = (dot(keys_t[...], score_ref[number], plain) * scaling).astype(jnp.bfloat16)
        for i, c in enumerate(columns):
            query_grad_ref[:, c] = query_grad[:, block_rows(i)].T
    own_grad_ref[:NODE_TOKENS, :] = key_total * scaling
    own_grad_ref[NODE_TOKENS:, :] = value_total


def finish(node, query, held, per_key, scaling):
    keys_s, scores, weights, scaled = held
    width = per_key * HEAD_SIZE
    seen_rows = (MAX_DEPTH + 1) * NODE_TOKENS
    vmem = pl.BlockSpec(memory_space=pltpu.VMEM)
    operands = (query, keys_s, scores[node], weights[node], scaled[node])
    pairs = per_key * NODE_TOKENS * seen_rows
    return pl.pallas_call(
        functools.partial(finish_kernel, node, per_key, scaling),
        out_shape=[
            pltpu.VMEM((NODE_TOKENS, width), jnp.bfloat16),
            pltpu.VMEM((2 * NODE_TOKENS, HEAD_SIZE), jnp.float32),
        ],
        in_specs=[vmem] * len(operands),
        out_specs=[vmem] * 2,
        scratch_shapes=[pltpu.VMEM((HEAD_SIZE, seen_rows), jnp.bfloat16)],
        compiler_params=pltpu.CompilerParams(vmem_limit_bytes=KERNEL_BYTES // 2),
        cost_estimate=pl.CostEstimate(
            flops=2 * pairs * HEAD_SIZE, transcendentals=0, bytes_accessed=2**20
        ),
    )(*[on_chip(a) for a in operands])


def on_chip(array):
    return pltpu.with_memory_space_constraint(array, pltpu.VMEM)


def attention(parents, place, queries, owns, grads, trunks, per_key, scaling):
    node_count = len(queries)
    group_count = trunks.shape[0]
    width = per_key * HEAD_SIZE
    tile_count = per_key // TILE_HEADS
    held_rows = (MAX_DEPTH + node_count) * NODE_TOKENS
    seen_rows = (MAX_DEPTH + 1) * NODE_TOKENS
    tile_rows = TILE_HEADS * NODE_TOKENS
    bf16, f32 = jnp.bfloat16, jnp.float32
    smem = pl.BlockSpec(memory_space=pltpu.SMEM)
    vmem = pl.BlockSpec(memory_space=pltpu.VMEM)
    half_shape = pltpu.VMEM((group_count // 2, 2 * NODE_TOKENS, HEAD_SIZE), bf16)
    out_shape = (
        [pltpu.VMEM((node_count * NODE_TOKENS, width), bf16), half_shape, half_shape]
        + [pltpu.VMEM((held_rows, HEAD_SIZE), bf16)]
        + [pltpu.VMEM((tile_count, seen_rows, tile_rows), bf16)] * node_count
        + [pltpu.VMEM((tile_count, NODE_TOKENS, tile_rows), bf16)] * node_count
        + [pltpu.VMEM((tile_count, HEAD_SIZE, tile_rows), bf16)] * node_count
    )
    pairs = node_count * per_key * NODE_TOKENS * seen_rows
    results = pl.pallas_call(
        functools.partial(attention_kernel, group_count, node_count, per_key, scaling),
        out_shape=out_shape,
        in_specs=[smem, smem] + [vmem] * (3 * node_count + 1),
        out_specs=[vmem] * len(out_shape),
        scratch_shapes=[
            pltpu.VMEM((held_rows, HEAD_SIZE), bf16),
            pltpu.VMEM((HEAD_SIZE, held_rows), bf16),
            pltpu.VMEM((2, seen_rows, tile_rows), f32),
            pltpu.VMEM((2, seen_rows, tile_rows), bf16),
            pltpu.VMEM((MAX_DEPTH * NODE_TOKENS, HEAD_SIZE), f32),
            pltpu.VMEM((MAX_DEPTH * NODE_TOKENS, HEAD_SIZE), f32),
        ],
        compiler_params=pltpu.CompilerParams(vmem_limit_bytes=KERNEL_BYTES),
        cost_estimate=pl.CostEstimate(
            flops=10 * pairs * HEAD_SIZE, transcendentals=pairs, bytes_accessed=8 * 2**20
        ),
    )(
        parents,
        place,
        *[on_chip(a) for a in (*queries, *owns, *grads, trunks)],
    )
    attended, near, far, keys_s = results[:4]
    scores, weights, scaled = [
        results[4 + i * node_count : 4 + (i + 1) * node_count] for i in range(3)
    ]
    return attended, (near, far), (keys_s, scores, weights, scaled)


def partner_pairs(count, bit):
    return [(i, i ^ bit) for i in range(count)]


def ring_pairs(count, shift):
    ring = ring_size(count)
    inner = count // ring
    return [(i, (i // inner + shift) % ring * inner + i % inner) for i in range(count)]


def gather_trunks(trunk, group_count):
    ring = ring_size(group_count)
    pieces = [trunk]
    for shift in range(1, ring):
        pieces.append(lax.ppermute(trunk, "leaf", ring_pairs(group_count, shift)))
    middle = (ring + 1) // 2
    held = jnp.stack(pieces)
    parts = [jnp.stack(pieces[:middle]), jnp.stack(pieces[middle:])] if ring > 1 else [held]
    for stage, bit in enumerate(exchange_bits(group_count // ring)):
        pairs = partner_pairs(group_count, bit)
        arrived = []
        for part in parts:
            arrived.append(lax.ppermute(part, "leaf", pairs))
        parts = [held, jnp.concatenate(arrived, axis=0)] if stage == 0 else [held]
        held = jnp.concatenate([held, *arrived], axis=0)
        if stage > 0:
            parts = [held]
    return held


def merged(near, arrived):
    return (near.astype(jnp.float32) + arrived.astype(jnp.float32)).astype(jnp.bfloat16)


def return_parts(near, far, group_count):
    ring = ring_size(group_count)
    middle = (ring + 1) // 2
    bits = exchange_bits(group_count // ring)
    for stage, bit in enumerate(reversed(bits)):
        pairs = partner_pairs(group_count, bit)
        if far.shape[0] == ring and ring > 1:
            late = lax.ppermute(far[middle:], "leaf", pairs)
            early = lax.ppermute(far[:middle], "leaf", pairs)
            late = merged(near[middle:], late)
            early, _ = lax.optimization_barrier((early, late))
            early = merged(near[:middle], early)
            blocks = [early[i] for i in range(middle)] + [late[i] for i in range(ring - middle)]
        elif stage == 0 and near.shape[0] > 1:
            half = near.shape[0] // 2
            early = lax.ppermute(far[half:], "leaf", pairs)
            late = lax.ppermute(far[:half], "leaf", pairs)
            far = merged(near[half:], early)
            late, _ = lax.optimization_barrier((late, far))
            near = merged(near[:half], late)
        else:
            arrived = lax.ppermute(far, "leaf", pairs)
            total = merged(near, arrived)
            half = near.shape[0] // 2
            near, far = total[:half], total[half:]
            blocks = [total[0]]
    total = blocks[0].astype(jnp.float32)
    for shift in range(1, ring):
        block = blocks[ring_order(shift)]
        arrived = lax.ppermute(block, "leaf", ring_pairs(group_count, shift))
        total = total + arrived.astype(jnp.float32)
    return total


def side_by_side_kernel(place_ref, mine_ref, came_ref, key_ref, value_ref):
    def write(left_ref, right_ref):
        for out_ref, rows in (
            (key_ref, slice(0, NODE_TOKENS)),
            (value_ref, slice(NODE_TOKENS, 2 * NODE_TOKENS)),
        ):
            out_ref[:, :HEAD_SIZE] = left_ref[rows, :]
            out_ref[:, HEAD_SIZE:] = right_ref[rows, :]

    first = place_ref[1] == 0
    pl.when(first)(lambda: write(mine_ref, came_ref))
    pl.when(jnp.logical_not(first))(lambda: write(came_ref, mine_ref))


def side_by_side(place, mine, came):
    vmem = pl.BlockSpec(memory_space=pltpu.VMEM)
    shape = jax.ShapeDtypeStruct((NODE_TOKENS, 2 * HEAD_SIZE), mine.dtype)
    return pl.pallas_call(
        side_by_side_kernel,
        out_shape=[shape, shape],
        in_specs=[pl.BlockSpec(memory_space=pltpu.SMEM), vmem, vmem],
        out_specs=[vmem, vmem],
        compiler_params=pltpu.CompilerParams(vmem_limit_bytes=KERNEL_BYTES // 8),
    )(place, on_chip(mine), on_chip(came))


def pair_of(arrays, columns):
    return jnp.concatenate([array[:, columns] for array in arrays], axis=0)


def paired_device(queries, keys, values, output_gradient, parents, per_key, scaling):
    group_count = lax.axis_size("leaf")
    my_head = lax.axis_index("head")
    my_group = lax.axis_index("leaf").astype(jnp.int32)
    width = output_gradient.shape[1]
    swap = [(0, 1), (1, 0)]
    first = my_head == 0
    other = 1 - my_head
    pair0 = pair_of((keys, values), slice(0, HEAD_SIZE))
    pair1 = pair_of((keys, values), slice(HEAD_SIZE, 2 * HEAD_SIZE))
    kept = jnp.where(first, pair0, pair1)
    came = lax.ppermute(jnp.where(first, pair1, pair0), "head", swap)
    query_send = lax.dynamic_slice_in_dim(queries, other * width, width, 1)
    query_kept = lax.dynamic_slice_in_dim(queries, my_head * width, width, 1)
    grads = [
        lax.dynamic_slice_in_dim(output_gradient, node * NODE_TOKENS, NODE_TOKENS, 0)
        for node in (my_head, other)
    ]
    query_came = lax.ppermute(query_send, "head", swap)
    trunks = gather_trunks(jnp.where(first, kept, came), group_count)
    place = jnp.stack([my_group, my_head, other]).astype(jnp.int32)
    query_nodes = [query_kept, query_came]
    attended, (near, far), held = attention(
        parents,
        place,
        query_nodes,
        [kept, came],
        grads,
        trunks,
        per_key,
        scaling,
    )
    query_away, own_away = finish(1, query_nodes[1], held, per_key, scaling)
    query_here, own_here = finish(0, query_nodes[0], held, per_key, scaling)
    query_back = lax.ppermute(query_away, "head", swap)
    total = return_parts(near, far, group_count)
    nothing = jnp.zeros_like(total)
    mine = (own_here + jnp.where(first, total, nothing)).astype(jnp.bfloat16)
    theirs = (own_away + jnp.where(first, nothing, total)).astype(jnp.bfloat16)
    came_back = lax.ppermute(theirs, "head", swap)
    key_home, value_home = side_by_side(place, mine, came_back)
    query_home = jnp.concatenate(
        [
            jnp.where(first, query_here, query_back),
            jnp.where(first, query_back, query_here),
        ],
        axis=1,
    )
    return (attended, query_home, key_home, value_home)


def general_device(queries, keys, values, output_gradient, parents, per_key, scaling):
    group_count = lax.axis_size("leaf")
    my_group = lax.axis_index("leaf").astype(jnp.int32)
    node_count = output_gradient.shape[0] // NODE_TOKENS
    query_all, key_all, value_all = [
        lax.all_to_all(a, "head", split_axis=1, concat_axis=0, tiled=True)
        for a in (queries, keys, values)
    ]
    spans = [slice(n * NODE_TOKENS, (n + 1) * NODE_TOKENS) for n in range(node_count)]
    owns = [jnp.concatenate([key_all[s], value_all[s]], axis=0) for s in spans]
    trunks = gather_trunks(owns[0], group_count)
    zero = my_group * 0
    place = [my_group]
    for node in range(node_count):
        place += [zero + node]
    query_nodes = [query_all[s] for s in spans]
    attended, (near, far), held = attention(
        parents,
        jnp.stack(place),
        query_nodes,
        owns,
        [output_gradient[s] for s in spans],
        trunks,
        per_key,
        scaling,
    )
    finished = [
        finish(node, query, held, per_key, scaling) for node, query in enumerate(query_nodes)
    ]
    query_grads = [query_grad for query_grad, _ in finished]
    own_grads = [own_grad for _, own_grad in finished]
    total = return_parts(near, far, group_count)
    grads = [own_grads[0] + total] + [own_grads[node] for node in range(1, node_count)]
    key_grad = jnp.concatenate([g[:NODE_TOKENS] for g in grads], axis=0).astype(jnp.bfloat16)
    value_grad = jnp.concatenate([g[NODE_TOKENS:] for g in grads], axis=0).astype(jnp.bfloat16)
    query_gradient = jnp.concatenate(query_grads, axis=0)
    query_home, key_home, value_home = [
        lax.all_to_all(a, "head", split_axis=0, concat_axis=1, tiled=True)
        for a in (query_gradient, key_grad, value_grad)
    ]
    return (attended, query_home, key_home, value_home)


def per_device(queries, keys, values, output_gradient, parents):
    node_count = output_gradient.shape[0] // NODE_TOKENS
    per_key = queries.shape[1] // keys.shape[1]
    scaling = 1.0 / math.sqrt(HEAD_SIZE)
    paired = lax.axis_size("head") == 2 and node_count == 2
    body = paired_device if paired else general_device
    return body(queries, keys, values, output_gradient, parents, per_key, scaling)


def solution(mesh):
    placed = (
        P(("leaf", "head"), None),
        P(("leaf", "head"), None),
        P(("leaf", "head"), None),
        P("leaf", "head"),
        P(),
    )
    return jax.shard_map(
        per_device,
        mesh=mesh,
        in_specs=placed,
        out_specs=(
            P("leaf", "head"),
            P(("leaf", "head"), None),
            P(("leaf", "head"), None),
            P(("leaf", "head"), None),
        ),
        check_vma=False,
    )
```
